8 devices in a mesh: dp: 2 (over z, y), fsdp: 4 (over x, core).
Axes of the slice: x: 2, y: 2, z: 1, core: 2. Of those that a mesh axis runs over, the one named last changes fastest.
Arguments:
- hidden: bfloat16 [8192, 512], P(('dp', 'fsdp')), parts along dimension 0
- targets: int32 [8192], P(('dp', 'fsdp')), parts along dimension 0
- weight: bfloat16 [32128, 512], P('fsdp')
Outputs:
- output 1: float32 [2], P('dp'), parts along dimension 0
- output 2: float32 [8192, 512], P(('dp', 'fsdp')), parts along dimension 0
- output 3: float32 [64256, 512], P(('dp', 'fsdp')), parts along dimension 0
There are 2 independent parts. The reference program is written for one: setup_inputs(seed, part) draws one part's arguments, and reference() takes and returns one part's arrays. A program takes and returns all parts, laid end to end along the dimension named above; an argument that names none is the same for every part.
All inputs are finite; a program needn't handle non-finite values.
Results may differ from the reference program's by a relative error of at most 0.001.
Values are sent between devices in bfloat16 or wider.
A program may use at most 1 GiB of HBM per device.

```python
import jax
import jax.numpy as jnp
from jax import lax

TOKENS = 4096
VOCAB = 32128
WIDTH = 512
BLOCKS = 4

BLOCK_ROWS = VOCAB // BLOCKS


def setup_inputs(seed: int = 0, part: int = 0) -> dict:
    base_key = jax.random.key(seed)
    key_hid, key_tgt, key_wgt = jax.random.split(base_key, 3)
    key_hid = jax.random.fold_in(key_hid, part)
    key_tgt = jax.random.fold_in(key_tgt, part)
    hidden = jax.random.normal(key_hid, (TOKENS, WIDTH), jnp.float32).astype(jnp.bfloat16)
    targets = jax.random.randint(key_tgt, (TOKENS,), 0, VOCAB, dtype=jnp.int32)
    weight = (jax.random.normal(key_wgt, (VOCAB, WIDTH), jnp.float32) * WIDTH ** -0.5).astype(jnp.bfloat16)
    return {"hidden": hidden, "targets": targets, "weight": weight}


def reference(hidden, targets, weight):
    w_blocks = weight.reshape(BLOCKS, BLOCK_ROWS, WIDTH)
    blk_starts = jnp.arange(BLOCKS, dtype=jnp.int32) * BLOCK_ROWS
    col_ids = jnp.arange(BLOCK_ROWS, dtype=jnp.int32)

    def block_logits(w_blk, blk_start):
        logits = jnp.dot(hidden, w_blk.T, preferred_element_type=jnp.float32)
        is_target = (targets - blk_start)[:, None] == col_ids[None, :]
        return logits, is_target

    def fwd_step(fwd_state, blk_pair):
        run_max, run_sum, tgt_logit = fwd_state
        logits, is_target = block_logits(blk_pair[0], blk_pair[1])
        new_max = jnp.maximum(run_max, jnp.max(logits, axis=1))
        run_sum = run_sum * jnp.exp(run_max - new_max) + jnp.sum(jnp.exp(logits - new_max[:, None]), axis=1)
        tgt_logit = tgt_logit + jnp.sum(jnp.where(is_target, logits, 0.0), axis=1)
        return (new_max, run_sum, tgt_logit), None

    init_state = (jnp.full((TOKENS,), -jnp.inf, jnp.float32), jnp.zeros((TOKENS,), jnp.float32), jnp.zeros((TOKENS,), jnp.float32))
    run_max, run_sum, tgt_logit = lax.scan(fwd_step, init_state, (w_blocks, blk_starts))[0]
    log_norm = run_max + jnp.log(run_sum)
    loss_val = (jnp.sum(log_norm - tgt_logit) / TOKENS).reshape(1)

    def bwd_step(dh_acc, blk_pair):
        logits, is_target = block_logits(blk_pair[0], blk_pair[1])
        dlogits = ((jnp.exp(logits - log_norm[:, None]) - is_target.astype(jnp.float32)) / TOKENS).astype(jnp.bfloat16)
        dh_acc = dh_acc + jnp.dot(dlogits, blk_pair[0], preferred_element_type=jnp.float32)
        dw_blk = jnp.dot(dlogits.T, hidden, preferred_element_type=jnp.float32)
        return dh_acc, dw_blk

    grad_hidden, dw_blocks = lax.scan(bwd_step, jnp.zeros((TOKENS, WIDTH), jnp.float32), (w_blocks, blk_starts))
    return loss_val, grad_hidden, dw_blocks.reshape(VOCAB, WIDTH)
```

```python
import jax
import jax.numpy as jnp
from jax import lax
from jax.experimental import pallas as pl
from jax.experimental.pallas import tpu as pltpu
from jax.sharding import PartitionSpec as P

SUB = 256
UNROLL_F = 14
UNROLL_B = 28
f32 = jnp.float32
bf16 = jnp.bfloat16


def _nn(a, b):
    return lax.dot_general(a, b, (((1,), (0,)), ((), ())), preferred_element_type=f32)


def _tn(a, b):
    return lax.dot_general(a, b, (((0,), (0,)), ((), ())), preferred_element_type=f32)


def _pipeline(step, steps, unroll):
    loops = (steps - 1) // unroll

    @pl.loop(0, loops)
    def _(i):
        for u in range(unroll):
            step(1 + i * unroll + u, (1 + u) % 2)

    for k in range(1 + loops * unroll, steps):
        step(k, k % 2)


def _fwd_kernel(w_ref, h_ref, m_ref, s_ref, ht, z0, z1, m8, s8):
    vloc, depth = w_ref.shape
    tok = h_ref.shape[0]
    full, rem = vloc // SUB, vloc % SUB
    zbuf = (z0, z1)

    def zdot(k, slot, rows=SUB):
        zbuf[slot][pl.ds(0, rows), :] = _nn(w_ref[pl.ds(k * SUB, rows), :], ht[...])

    def epi(slot, rows=SUB):
        z = zbuf[slot][pl.ds(0, rows), :].reshape(rows // 8, 8, tok)
        old = m8[...]
        new = jnp.maximum(old, jnp.max(z, axis=0))
        s8[...] = s8[...] * jnp.exp(old - new) + jnp.sum(jnp.exp(z - new[None]), axis=0)
        m8[...] = new

    ht[...] = h_ref[...].T
    m8[...] = jnp.full(m8.shape, -jnp.inf, f32)
    s8[...] = jnp.zeros(s8.shape, f32)

    def step(k, par, zrows=SUB, erows=SUB):
        if zrows:
            zdot(k + 1, 1 - par, zrows)
        if erows:
            epi(par, erows)

    zdot(0, 0)
    step(0, 0)
    _pipeline(step, full - 1, UNROLL_F)
    step(full - 1, (full - 1) % 2, zrows=rem)
    if rem:
        step(full, full % 2, zrows=0, erows=rem)
    top = jnp.max(m8[...], axis=0, keepdims=True)
    m_ref[...] = top
    s_ref[...] = jnp.sum(s8[...] * jnp.exp(m8[...] - top), axis=0, keepdims=True)


def _bwd_kernel(w_ref, h_ref, lse_ref, tgt_ref, dw_ref, dh_ref, zt_ref, ht, dht, z0, z1, g0, g1):
    chunk = pl.program_id(0)
    vloc, depth = w_ref.shape
    tok = h_ref.shape[0]
    full, rem = vloc // SUB, vloc % SUB
    zbuf, gbuf = (z0, z1), (g0, g1)
    scale = 1.0 / (tok * pl.num_programs(0))

    def zdot(k, slot, rows=SUB):
        zbuf[slot][pl.ds(0, rows), :] = _nn(w_ref[pl.ds(k * SUB, rows), :], ht[...])

    def epi(k, slot, rows=SUB):
        z = zbuf[slot][pl.ds(0, rows), :]
        hit = lax.broadcasted_iota(jnp.int32, (rows, tok), 0) == tgt_ref[...] - k * SUB
        p = jnp.exp(z - lse_ref[...])
        zt_ref[...] += jnp.sum(jnp.where(hit, z, 0.0), axis=0, keepdims=True)
        gbuf[slot][pl.ds(0, rows), :] = ((p - jnp.where(hit, 1.0, 0.0)) * (1.0 / 4096.0)).astype(bf16)

    def ddot(k, slot, rows=SUB):
        g = gbuf[slot][pl.ds(0, rows), :]
        rng = pl.ds(k * SUB, rows)
        dw_ref[rng, :] = dw_ref[rng, :] + _nn(g, h_ref[...])
        dht[...] += _tn(w_ref[rng, :], g)

    @pl.when(chunk == 0)
    def _():
        @pl.loop(0, vloc // 32)
        def _(i):
            dw_ref[pl.ds(i * 32, 32), :] = jnp.zeros((32, depth), f32)

    ht[...] = h_ref[...].T
    dht[...] = jnp.zeros(dht.shape, f32)
    zt_ref[...] = jnp.zeros(zt_ref.shape, f32)

    def step(k, par, zrows=SUB, erows=SUB, drows=SUB):
        if drows:
            ddot(k - 1, 1 - par, drows)
        if zrows:
            zdot(k + 1, 1 - par, zrows)
        if erows:
            epi(k, par, erows)

    zdot(0, 0)
    step(0, 0, drows=0)
    _pipeline(step, full - 1, UNROLL_B)
    step(full - 1, (full - 1) % 2, zrows=rem)
    step(full, full % 2, zrows=0, erows=rem)
    if rem:
        step(full + 1, (full + 1) % 2, zrows=0, erows=0, drows=rem)
    dh_ref[...] = dht[...].T


def solution(mesh):
    groups = mesh.shape["fsdp"]
    tok_spec = P(("dp", "fsdp"), None)

    def local_head(hidden, targets, weight):
        tok, depth = hidden.shape
        vloc = weight.shape[0]
        total = tok * groups
        rank = lax.axis_index("fsdp")
        h_all = lax.all_gather(hidden, "fsdp", axis=0, tiled=True)
        t_all = lax.all_gather(targets, "fsdp", axis=0, tiled=True)
        row = lambda c: (0, c)
        whole = lambda c: (0, 0)
        params = pltpu.CompilerParams(vmem_limit_bytes=66_000_000, dimension_semantics=("arbitrary",))
        m, s = pl.pallas_call(
            _fwd_kernel,
            grid=(groups,),
            in_specs=[pl.BlockSpec((vloc, depth), whole), pl.BlockSpec((tok, depth), lambda c: (c, 0))],
            out_specs=[pl.BlockSpec((1, tok), row)] * 2,
            out_shape=[jax.ShapeDtypeStruct((1, total), f32)] * 2,
            scratch_shapes=[pltpu.VMEM((depth, tok), bf16)] + [pltpu.VMEM((SUB, tok), f32)] * 2 + [pltpu.VMEM((8, tok), f32)] * 2,
            compiler_params=params,
            name="ce_fwd",
        )(weight, h_all)
        ms = lax.all_gather(jnp.concatenate([m, s], axis=0), "fsdp")
        top = jnp.max(ms[:, 0], axis=0)
        lse = top + jnp.log(jnp.sum(ms[:, 1] * jnp.exp(ms[:, 0] - top), axis=0))
        dw, dh, zt = pl.pallas_call(
            _bwd_kernel,
            grid=(groups,),
            in_specs=[
                pl.BlockSpec((vloc, depth), whole),
                pl.BlockSpec((tok, depth), lambda c: (c, 0)),
                pl.BlockSpec((1, tok), row),
                pl.BlockSpec((1, tok), row),
            ],
            out_specs=[pl.BlockSpec((vloc, depth), whole), pl.BlockSpec((tok, depth), lambda c: (c, 0)), pl.BlockSpec((1, tok), row)],
            out_shape=[
                jax.ShapeDtypeStruct((vloc, depth), f32),
                jax.ShapeDtypeStruct((total, depth), f32),
                jax.ShapeDtypeStruct((1, total), f32),
            ],
            scratch_shapes=[pltpu.VMEM((depth, tok), bf16), pltpu.VMEM((depth, tok), f32)]
            + [pltpu.VMEM((SUB, tok), f32)] * 2
            + [pltpu.VMEM((SUB, tok), bf16)] * 2,
            compiler_params=params,
            name="ce_bwd",
        )(weight, h_all, lse[None, :], (t_all - rank * vloc)[None, :])
        grad_h = lax.psum_scatter(dh, "fsdp", scatter_dimension=0, tiled=True)
        loss = lax.psum(jnp.sum(lse) / groups - jnp.sum(zt), "fsdp") / total
        return loss.reshape(1), grad_h, dw

    return jax.shard_map(local_head, mesh=mesh, in_specs=(tok_spec, P(("dp", "fsdp")), P("fsdp", None)), out_specs=(P("dp"), tok_spec, tok_spec), check_vma=False)
```

```python
import jax
import jax.numpy as jnp
from jax import lax
from jax.experimental import pallas as pl
from jax.experimental.pallas import tpu as pltpu
from jax.sharding import PartitionSpec as P

SUB = 256
UN_F = 14
UN_B = 14
f32 = jnp.float32
bf16 = jnp.bfloat16
MESH = pl.DeviceIdType.MESH


def _nn(a, b):
    return lax.dot_general(a, b, (((1,), (0,)), ((), ())), preferred_element_type=f32)


def _tn(a, b):
    return lax.dot_general(a, b, (((0,), (0,)), ((), ())), preferred_element_type=f32)


def _pieces(full, rem, unroll):
    loops = (full - 2) // unroll
    cuts = [0, 2 * SUB] + [(2 + (i + 1) * unroll) * SUB for i in range(loops)] + [full * SUB + rem]
    return [(a, b - a) for a, b in zip(cuts[:-1], cuts[1:])]


def _fwd_chunk(w, h, ht, zb, mb, s8, tgt=None, zt8=None, mid=None, need=None):
    vloc = w.shape[0]
    tok = h.shape[0]
    full, rem = vloc // SUB, vloc % SUB
    loops = (full - 2) // UN_F
    ht[...] = h[...].T
    mb[1][...] = jnp.full(mb[1].shape, -jnp.inf, f32)
    s8[...] = jnp.zeros(s8.shape, f32)

    def zdot(k, slot, rows=SUB):
        z = _nn(w[pl.ds(k * SUB, rows), :], ht[...])
        zb[slot][pl.ds(0, rows), :] = z
        mb[slot][...] = jnp.maximum(mb[1 - slot][...], jnp.max(z.reshape(rows // 8, 8, tok), axis=0))

    def epi(k, slot, rows=SUB):
        z = zb[slot][pl.ds(0, rows), :].reshape(rows // 8, 8, tok)
        new = mb[slot][...]
        s8[...] = s8[...] * jnp.exp(mb[2][...] - new) + jnp.sum(jnp.exp(z - new[None]), axis=0)
        mb[2][...] = new
        if tgt is not None:
            t = tgt - k * SUB
            lane = lax.broadcasted_iota(jnp.int32, (8, tok), 0)
            acc = zt8[...]
            for r in range(rows // 8):
                acc = jnp.where(lane + r * 8 == t, z[r], acc)
            zt8[...] = acc

    def step(k, par, zrows=SUB, erows=SUB):
        if zrows:
            zdot(k + 1, 1 - par, zrows)
        if erows:
            epi(k, par, erows)

    mb[2][...] = mb[1][...]
    if need is not None:
        need(0)
    zdot(0, 0)
    step(0, 0)

    @pl.loop(0, loops)
    def _(i):
        if need is not None:
            for n in range(loops):
                pl.when(i == n)(lambda n=n: need(1 + n))
        for u in range(UN_F):
            step(1 + i * UN_F + u, (1 + u) % 2)
        if mid is not None:
            pl.when(i == 0)(mid)

    if need is not None:
        need(1 + loops)
    for k in range(1 + loops * UN_F, full - 1):
        step(k, k % 2)
    step(full - 1, (full - 1) % 2, zrows=rem)
    step(full, full % 2, zrows=0, erows=rem)
    m8 = mb[2][...]
    top = jnp.max(m8, axis=0, keepdims=True)
    return top + jnp.log(jnp.sum(s8[...] * jnp.exp(m8 - top), axis=0, keepdims=True))


def _bwd_chunk(w, h, ht, lse, tgt, dw, dht, zb, gb, zt8=None, mid=None, need=None, done=None, scale=1.0):
    vloc = w.shape[0]
    tok = h.shape[0]
    full, rem = vloc // SUB, vloc % SUB
    loops = (full - 2) // UN_B

    def zdot(k, slot, rows=SUB):
        zb[slot][pl.ds(0, rows), :] = _nn(w[pl.ds(k * SUB, rows), :], ht[...])

    def epi(k, slot, rows=SUB):
        z = zb[slot][pl.ds(0, rows), :]
        hit = lax.broadcasted_iota(jnp.int32, (rows, tok), 0) == tgt[...] - k * SUB
        p = jnp.exp(z - lse[...])
        if zt8 is not None:
            zt8[...] += jnp.sum(jnp.where(hit, z, 0.0).reshape(rows // 8, 8, tok), axis=0)
        gb[slot][pl.ds(0, rows), :] = ((p - jnp.where(hit, 1.0, 0.0)) * scale).astype(bf16)

    def ddot(k, slot, rows=SUB):
        g = gb[slot][pl.ds(0, rows), :]
        rng = pl.ds(k * SUB, rows)
        dw[rng, :] = dw[rng, :] + _nn(g, h[...])
        dht[...] += _tn(w[rng, :], g)

    def step(k, par, zrows=SUB, erows=SUB, drows=SUB):
        if drows:
            ddot(k - 1, 1 - par, drows)
        if zrows:
            zdot(k + 1, 1 - par, zrows)
        if erows:
            epi(k, par, erows)

    dht[...] = jnp.zeros(dht.shape, f32)
    if need is not None:
        need(0)
    zdot(0, 0)
    step(0, 0, drows=0)
    if mid is not None:
        mid()

    @pl.loop(0, loops)
    def _(i):
        if need is not None:
            for n in range(loops):
                pl.when(i == n)(lambda n=n: need(1 + n))
        for u in range(UN_B):
            step(1 + i * UN_B + u, (1 + u) % 2)
        if done is not None:
            for n in range(loops):
                done(n, i == n)

    if need is not None:
        need(1 + loops)
    for k in range(1 + loops * UN_B, full - 1):
        step(k, k % 2)
    step(full - 1, (full - 1) % 2, zrows=rem)
    step(full, full % 2, zrows=0, erows=rem)
    step(full + 1, (full + 1) % 2, zrows=0, erows=0, drows=rem)
    if done is not None:
        done(loops, None)


def _done_pieces(vloc):
    full = vloc // SUB
    loops = (full - 2) // UN_B
    cuts = [0] + [(i + 1) * UN_B * SUB for i in range(loops)] + [vloc]
    return [(a, b - a) for a, b in zip(cuts[:-1], cuts[1:])]


def _exchange_kernel(total, h_in, t_in, w_in, dwp, x_out, s_out, lse_out, loss_out,
                     w, hc, ht, dw, dht, part, ring, tg, lst, zs, lsec, z0, z1, g0, g1, ma, mb_, mc, s8, zt8, ztf,
                     wsem, lsem, hsend, hrecv, tsend, trecv, stsend, strecv, psend, precv, zsend, zrecv, osem):
    vloc, depth = w_in.shape
    tok = h_in.shape[0]
    half = tok // 2
    me = lax.axis_index("fsdp")
    chip, core = me // 2, me % 2
    sib = 2 * chip + (1 - core)
    far = 2 * (1 - chip) + core
    fars = [2 * (1 - chip), 2 * (1 - chip) + 1]
    base = me * vloc
    dev = lambda d: {"fsdp": d}
    zb, gb, mb = (z0, z1), (g0, g1), (ma, mb_, mc)
    scale = 1.0 / total

    def rcopy(src, dst, ssem, rsem, d):
        return pltpu.make_async_remote_copy(src_ref=src, dst_ref=dst, send_sem=ssem, recv_sem=rsem, device_id=dev(d), device_id_type=MESH)

    def wait_bytes(ref, sem):
        pltpu.make_async_copy(ref, ref, sem).wait()

    pieces = _pieces(vloc // SUB, vloc % SUB, UN_F)
    wcopy = [pltpu.make_async_copy(w_in.at[pl.ds(a, n), :], w.at[pl.ds(a, n), :], wsem.at[i]) for i, (a, n) in enumerate(pieces)]
    own_h = pltpu.make_async_copy(h_in, hc.at[0], lsem.at[0])
    own_t = pltpu.make_async_copy(t_in, tg.at[pl.ds(0, 2)], lsem.at[1])
    own_h.start()
    own_t.start()
    for c in wcopy:
        c.start()

    barrier = pltpu.get_barrier_semaphore()
    for d in [sib] + fars:
        pl.semaphore_signal(barrier, inc=1, device_id=dev(d), device_id_type=MESH)
    pl.semaphore_wait(barrier, 3)

    mine = pl.ds(core * half, half)
    send_sib = rcopy(h_in, hc.at[1], hsend.at[0], hrecv.at[0], sib)
    send_far = [rcopy(h_in.at[pl.ds(i * half, half), :], hc.at[2 + i, mine, :], hsend.at[1 + i], hrecv.at[1 + i], far) for i in range(2)]
    relay = [rcopy(hc.at[2 + i, mine, :], hc.at[2 + i, mine, :], hsend.at[3 + i], hrecv.at[3 + i], sib) for i in range(2)]
    send_sib.start()
    for c in send_far:
        c.start()
    rcopy(t_in, tg.at[pl.ds(2, 2)], tsend, trecv, sib).start()
    for d in fars:
        for i in range(2):
            rcopy(t_in.at[pl.ds(i, 1)], tg.at[pl.ds(4 + 2 * i + core, 1)], tsend, trecv, d).start()

    @pl.loop(0, vloc // 32)
    def _(i):
        dw[pl.ds(i * 32, 32), :] = jnp.zeros((32, depth), f32)

    zt8[...] = jnp.zeros(zt8.shape, f32)
    ztf[...] = jnp.zeros(ztf.shape, f32)

    def put_stat(pos, v):
        for i in range(2):
            lst[me * 8 + pos * 2 + i] = v[:, i * half:(i + 1) * half]

    def send_stat(pos):
        def go(row, dst_pos, dst_half, d):
            rcopy(lst.at[pl.ds(me * 8 + row, 1)], lst.at[pl.ds(me * 8 + dst_pos * 2 + dst_half, 1)], stsend, strecv.at[dst_pos], d).start()

        near = pos < 2
        for i in range(2):
            go(pos * 2 + i, jnp.where(near, 1 - pos, pos), i, sib)
            for k in range(2):
                go(
                    pos * 2 + i,
                    jnp.where(near, 2 + i, jnp.where(k == i, 0, 1)),
                    jnp.where(near, jnp.where(pos == 0, core, 1 - core), pos - 2),
                    fars[k],
                )

    own_h.wait()
    own_t.wait()
    tg0 = jnp.concatenate([tg[0], tg[1]], axis=1) - base
    put_stat(0, _fwd_chunk(w, hc.at[0], ht.at[0], zb, mb, s8, tgt=tg0, zt8=ztf, need=lambda n: wcopy[n].wait()))
    send_stat(0)

    @pl.loop(1, 4)
    def _(pos):
        @pl.when(pos == 1)
        def _():
            send_sib.wait_recv()

        for i in range(2):
            @pl.when(pos == 2 + i)
            def _():
                relay[i].wait_recv()

        def forward():
            for i in range(2):
                @pl.when(pos == 1 + i)
                def _():
                    send_far[i].wait_recv()
                    relay[i].start()

        put_stat(pos, _fwd_chunk(w, hc.at[pos], ht.at[pos], zb, mb, s8, mid=forward))
        send_stat(pos)

    wait_bytes(tg.at[pl.ds(2, 6)], trecv)

    def join_stat(pos):
        rows = [[lst[s * 8 + pos * 2 + i] for s in range(4)] for i in range(2)]
        out = []
        for r in rows:
            top = jnp.maximum(jnp.maximum(r[0], r[1]), jnp.maximum(r[2], r[3]))
            out.append(top + jnp.log(sum(jnp.exp(x - top) for x in r)))
        return jnp.concatenate(out, axis=1)

    dpieces = _done_pieces(vloc)
    flush = [pltpu.make_async_copy(dw.at[pl.ds(a, n), :], dwp.at[pl.ds(a, n), :], osem.at[i]) for i, (a, n) in enumerate(dpieces)]
    theirs = pl.ds((1 - core) * half, half)
    swap = [rcopy(part.at[i, theirs, :], ring.at[i], psend.at[i], precv.at[i], sib) for i in range(2)]
    cross = [rcopy(part.at[i, mine, :], x_out.at[pl.ds(i * half, half), :], psend.at[2 + i], precv.at[2 + i], far) for i in range(2)]
    last = rcopy(part.at[2], s_out, psend.at[4], precv.at[4], sib)

    lsum = jnp.zeros((1, tok), f32)

    @pl.loop(0, 3)
    def _(i):
        pos = lax.rem(i + 1, 3) + 1
        for q in range(3):
            @pl.when(i == q)
            def _():
                wait_bytes(lst.at[pl.ds(0, 6)], strecv.at[(2, 3, 1)[q]])

        lse = join_stat(pos)
        lsec[pl.ds(pos, 1)] = lse[None]
        tpos = jnp.concatenate([tg[pos * 2], tg[pos * 2 + 1]], axis=1) - base

        def combine():
            for q in range(2):
                @pl.when(i == q + 1)
                def _():
                    swap[q].wait_recv()
                    for j in range(4):
                        rows = pl.ds(core * half + j * (half // 4), half // 4)
                        part[q, rows, :] += ring[q, pl.ds(j * (half // 4), half // 4), :]
                    cross[q].start()

        def done(n, cond):
            pl.when(i == 2 if cond is None else jnp.logical_and(cond, i == 2))(lambda: flush[n].start())

        _bwd_chunk(w, hc.at[pos], ht.at[pos], lse, tpos, dw, dht, zb, gb, zt8=zt8, mid=combine, done=done, scale=scale)
        part[i] = dht[...].T
        for q in range(2):
            pl.when(i == q)(lambda q=q: swap[q].start())

    last.start()
    wait_bytes(lst.at[pl.ds(0, 6)], strecv.at[0])
    lsec[0] = join_stat(0)
    lse_out[...] = lsec[0]
    zsum = jnp.sum(zt8[...] + ztf[...], keepdims=True)
    zs[me] = jnp.broadcast_to(zsum, (1, 128))
    for d in [sib] + fars:
        rcopy(zs.at[pl.ds(me, 1)], zs.at[pl.ds(me, 1)], zsend, zrecv, d).start()
    lsum = jnp.sum(lsec[0] + lsec[1] + lsec[2] + lsec[3], keepdims=True)
    wait_bytes(zs.at[pl.ds(0, 3)], zrecv)
    loss_out[...] = (lsum - (zs[0] + zs[1] + zs[2] + zs[3])) * scale
    wait_bytes(zs.at[pl.ds(0, 3)], zsend)
    wait_bytes(lst.at[pl.ds(0, 24)], stsend)
    wait_bytes(tg.at[pl.ds(0, 6)], tsend)
    for c in [send_sib] + send_far + relay + swap:
        c.wait_send()
    for c in flush:
        c.wait()
    for c in cross + [last]:
        c.wait()


def _own_kernel(total, w_in, h_ref, t_ref, lse_ref, dwp, x_ref, s_ref, dwo, dh_ref,
                w, ht, dw, dht, z0, z1, g0, g1, wsem, dsem, osem):
    vloc, depth = w_in.shape
    pieces = _pieces(vloc // SUB, vloc % SUB, UN_B)
    dpieces = _done_pieces(vloc)
    wcopy = [pltpu.make_async_copy(w_in.at[pl.ds(a, n), :], w.at[pl.ds(a, n), :], wsem.at[i]) for i, (a, n) in enumerate(pieces)]
    dcopy = [pltpu.make_async_copy(dwp.at[pl.ds(a, n), :], dw.at[pl.ds(a, n), :], dsem.at[i]) for i, (a, n) in enumerate(dpieces)]
    flush = [pltpu.make_async_copy(dw.at[pl.ds(a, n), :], dwo.at[pl.ds(a, n), :], osem.at[i]) for i, (a, n) in enumerate(dpieces)]
    wcopy[0].start()
    wcopy[1].start()
    for i in range(len(dpieces)):
        dcopy[i].start()
        if i + 2 < len(wcopy):
            wcopy[i + 2].start()
    ht[...] = h_ref[...].T

    def need(n):
        wcopy[n].wait()
        if n > 0:
            dcopy[n - 1].wait()

    def done(n, cond):
        if cond is None:
            flush[n].start()
        else:
            pl.when(cond)(lambda: flush[n].start())

    _bwd_chunk(w, h_ref, ht, lse_ref, t_ref, dw, dht, (z0, z1), (g0, g1), need=need, done=done, scale=1.0 / total)
    dh_ref[...] = dht[...].T + (x_ref[...] + s_ref[...])
    for c in flush:
        c.wait()


def solution(mesh):
    groups = mesh.shape["fsdp"]
    tok_spec = P(("dp", "fsdp"), None)

    def local_head(hidden, targets, weight):
        tok, depth = hidden.shape
        vloc = weight.shape[0]
        total = tok * groups
        half = tok // 2
        vm = pltpu.VMEM
        dma = pltpu.SemaphoreType.DMA
        hbm = pl.BlockSpec(memory_space=pl.ANY)
        loc = pl.BlockSpec(memory_space=pltpu.VMEM)
        np_f = len(_pieces(vloc // SUB, vloc % SUB, UN_F))
        np_b = len(_pieces(vloc // SUB, vloc % SUB, UN_B))
        nd = len(_done_pieces(vloc))
        sds = jax.ShapeDtypeStruct
        dwp, x, s, lse, loss = pl.pallas_call(
            lambda *refs: _exchange_kernel(total, *refs),
            in_specs=[hbm, hbm, hbm],
            out_specs=[hbm, hbm, hbm, loc, loc],
            out_shape=[sds((vloc, depth), f32), sds((tok, depth), f32), sds((tok, depth), f32), sds((1, tok), f32), sds((1, 128), f32)],
            scratch_shapes=[
                vm((vloc, depth), bf16), vm((groups, tok, depth), bf16), vm((groups, depth, tok), bf16), vm((vloc, depth), f32),
                vm((depth, tok), f32), vm((3, tok, depth), f32), vm((2, half, depth), f32),
                vm((8, 1, half), jnp.int32), vm((32, 1, half), f32), vm((4, 1, 128), f32), vm((4, 1, tok), f32),
                vm((SUB, tok), f32), vm((SUB, tok), f32), vm((SUB, tok), bf16), vm((SUB, tok), bf16),
                vm((8, tok), f32), vm((8, tok), f32), vm((8, tok), f32), vm((8, tok), f32), vm((8, tok), f32), vm((8, tok), f32),
                dma((np_f,)), dma((2,)), dma((5,)), dma((5,)), dma, dma, dma, dma((4,)), dma((5,)), dma((5,)), dma, dma, dma((nd,)),
            ],
            compiler_params=pltpu.CompilerParams(vmem_limit_bytes=66_500_000, collective_id=0, has_side_effects=True),
            name="ce_exchange",
        )(hidden, targets.reshape(2, 1, half), weight)
        mine = (targets - lax.axis_index("fsdp") * vloc)[None, :]
        dw, dh = pl.pallas_call(
            lambda *refs: _own_kernel(total, *refs),
            in_specs=[hbm, loc, loc, loc, hbm, loc, loc],
            out_specs=[hbm, loc],
            out_shape=[sds((vloc, depth), f32), sds((tok, depth), f32)],
            scratch_shapes=[
                vm((vloc, depth), bf16), vm((depth, tok), bf16), vm((vloc, depth), f32), vm((depth, tok), f32),
                vm((SUB, tok), f32), vm((SUB, tok), f32), vm((SUB, tok), bf16), vm((SUB, tok), bf16),
                dma((np_b,)), dma((nd,)), dma((nd,)),
            ],
            compiler_params=pltpu.CompilerParams(vmem_limit_bytes=66_500_000),
            name="ce_own",
        )(weight, hidden, mine, lse, dwp, x, s)
        return loss[0, :1], dh, dw

    return jax.shard_map(local_head, mesh=mesh, in_specs=(tok_spec, P(("dp", "fsdp")), P("fsdp", None)), out_specs=(P("dp"), tok_spec, tok_spec), check_vma=False)
```

```python
import jax
import jax.numpy as jnp
from jax import lax
from jax.experimental import pallas as pl
from jax.experimental.pallas import tpu as pltpu
from jax.sharding import PartitionSpec as P

SUB = 256
UN_O = 4
UN_F = 14
UN_B = 14
UN_L = 4
f32 = jnp.float32
bf16 = jnp.bfloat16
MESH = pl.DeviceIdType.MESH


def _nn(a, b):
    return lax.dot_general(a, b, (((1,), (0,)), ((), ())), preferred_element_type=f32)


def _tn(a, b):
    return lax.dot_general(a, b, (((0,), (0,)), ((), ())), preferred_element_type=f32)


def _pieces(full, rem, unroll):
    loops = (full - 2) // unroll
    cuts = [0, 2 * SUB] + [(2 + (i + 1) * unroll) * SUB for i in range(loops)] + [full * SUB + rem]
    return [(a, b - a) for a, b in zip(cuts[:-1], cuts[1:])]


def _fwd_chunk(w, h, ht, zb, mb, s8, un, tgt=None, zt8=None, mid=None, need=None, clear=None):
    vloc = w.shape[0]
    tok = h.shape[0]
    full, rem = vloc // SUB, vloc % SUB
    loops = (full - 2) // un
    ht[...] = h[...].T
    mb[1][...] = jnp.full(mb[1].shape, -jnp.inf, f32)
    s8[...] = jnp.zeros(s8.shape, f32)

    def zdot(k, slot, rows=SUB):
        z = _nn(w[pl.ds(k * SUB, rows), :], ht[...])
        zb[slot][pl.ds(0, rows), :] = z
        mb[slot][...] = jnp.maximum(mb[1 - slot][...], jnp.max(z.reshape(rows // 8, 8, tok), axis=0))

    def epi(k, slot, rows=SUB):
        z = zb[slot][pl.ds(0, rows), :].reshape(rows // 8, 8, tok)
        new = mb[slot][...]
        s8[...] = s8[...] * jnp.exp(mb[2][...] - new) + jnp.sum(jnp.exp(z - new[None]), axis=0)
        mb[2][...] = new
        if clear is not None:
            clear[pl.ds(k * SUB, rows), :] = jnp.zeros((rows, clear.shape[1]), f32)
        if tgt is not None:
            t = tgt - k * SUB
            lane = lax.broadcasted_iota(jnp.int32, (8, tok), 0)
            acc = zt8[...]
            for r in range(rows // 8):
                acc = jnp.where(lane + r * 8 == t, z[r], acc)
            zt8[...] = acc

    def step(k, par, zrows=SUB, erows=SUB):
        if zrows:
            zdot(k + 1, 1 - par, zrows)
        if erows:
            epi(k, par, erows)

    mb[2][...] = mb[1][...]
    if need is not None:
        need(0)
    zdot(0, 0)
    step(0, 0)

    @pl.loop(0, loops)
    def _(i):
        if need is not None:
            for n in range(loops):
                pl.when(i == n)(lambda n=n: need(1 + n))
        for u in range(un):
            step(1 + i * un + u, (1 + u) % 2)
        if mid is not None:
            pl.when(i == 0)(mid)

    if need is not None:
        need(1 + loops)
    for k in range(1 + loops * un, full - 1):
        step(k, k % 2)
    step(full - 1, (full - 1) % 2, zrows=rem)
    step(full, full % 2, zrows=0, erows=rem)
    m8 = mb[2][...]
    top = jnp.max(m8, axis=0, keepdims=True)
    return top + jnp.log(jnp.sum(s8[...] * jnp.exp(m8 - top), axis=0, keepdims=True))


def _bwd_chunk(w, h, ht, lse, tgt, dw, dht, zb, gb, un, zt8=None, mid=None, need=None, done=None, scale=1.0):
    vloc = w.shape[0]
    tok = h.shape[0]
    full, rem = vloc // SUB, vloc % SUB
    loops = (full - 2) // un

    def zdot(k, slot, rows=SUB):
        zb[slot][pl.ds(0, rows), :] = _nn(w[pl.ds(k * SUB, rows), :], ht[...])

    def epi(k, slot, rows=SUB):
        z = zb[slot][pl.ds(0, rows), :]
        hit = lax.broadcasted_iota(jnp.int32, (rows, tok), 0) == tgt[...] - k * SUB
        p = jnp.exp(z - lse[...])
        if zt8 is not None:
            zt8[...] += jnp.sum(jnp.where(hit, z, 0.0).reshape(rows // 8, 8, tok), axis=0)
        gb[slot][pl.ds(0, rows), :] = ((p - jnp.where(hit, 1.0, 0.0)) * scale).astype(bf16)

    def ddot(k, slot, rows=SUB):
        g = gb[slot][pl.ds(0, rows), :]
        rng = pl.ds(k * SUB, rows)
        dw[rng, :] = dw[rng, :] + _nn(g, h[...])
        dht[...] += _tn(w[rng, :], g)

    def step(k, par, zrows=SUB, erows=SUB, drows=SUB):
        if drows:
            ddot(k - 1, 1 - par, drows)
        if zrows:
            zdot(k + 1, 1 - par, zrows)
        if erows:
            epi(k, par, erows)

    dht[...] = jnp.zeros(dht.shape, f32)
    if need is not None:
        need(0)
    zdot(0, 0)
    step(0, 0, drows=0)
    if mid is not None:
        mid()

    @pl.loop(0, loops)
    def _(i):
        if need is not None:
            for n in range(loops):
                pl.when(i == n)(lambda n=n: need(1 + n))
        for u in range(un):
            step(1 + i * un + u, (1 + u) % 2)
        if done is not None:
            for n in range(loops):
                done(n, i == n)

    if need is not None:
        need(1 + loops)
    for k in range(1 + loops * un, full - 1):
        step(k, k % 2)
    step(full - 1, (full - 1) % 2, zrows=rem)
    step(full, full % 2, zrows=0, erows=rem)
    step(full + 1, (full + 1) % 2, zrows=0, erows=0, drows=rem)
    if done is not None:
        done(loops, None)


def _done_pieces(vloc, un):
    full = vloc // SUB
    loops = (full - 2) // un
    cuts = [0] + [(i + 1) * un * SUB for i in range(loops)] + [vloc]
    return [(a, b - a) for a, b in zip(cuts[:-1], cuts[1:])]


def _exchange_kernel(total, h_in, t_in, w_in, dwp, x_out, s_out, lse_out, loss_out,
                     w, hc, ht, dw, dht, part, ring, tg, lst, zs, lsec, z0, z1, g0, g1, ma, mb_, mc, s8, zt8, ztf,
                     wsem, lsem, hsend, hrecv, tsend, trecv, stsend, strecv, psend, precv, zsend, zrecv, osem):
    vloc, depth = w_in.shape
    tok = h_in.shape[0]
    half = tok // 2
    me = lax.axis_index("fsdp")
    chip, core = me // 2, me % 2
    sib = 2 * chip + (1 - core)
    far = 2 * (1 - chip) + core
    fars = [2 * (1 - chip), 2 * (1 - chip) + 1]
    base = me * vloc
    dev = lambda d: {"fsdp": d}
    zb, gb, mb = (z0, z1), (g0, g1), (ma, mb_, mc)
    scale = 1.0 / total

    def rcopy(src, dst, ssem, rsem, d):
        return pltpu.make_async_remote_copy(src_ref=src, dst_ref=dst, send_sem=ssem, recv_sem=rsem, device_id=dev(d), device_id_type=MESH)

    def wait_bytes(ref, sem):
        pltpu.make_async_copy(ref, ref, sem).wait()

    pieces = _pieces(vloc // SUB, vloc % SUB, UN_O)
    wcopy = [pltpu.make_async_copy(w_in.at[pl.ds(a, n), :], w.at[pl.ds(a, n), :], wsem.at[i]) for i, (a, n) in enumerate(pieces)]
    own_h = pltpu.make_async_copy(h_in, hc.at[0], lsem.at[0])
    own_t = pltpu.make_async_copy(t_in, tg.at[pl.ds(0, 2)], lsem.at[1])
    own_h.start()
    own_t.start()
    for c in wcopy:
        c.start()

    barrier = pltpu.get_barrier_semaphore()
    for d in [sib] + fars:
        pl.semaphore_signal(barrier, inc=1, device_id=dev(d), device_id_type=MESH)
    pl.semaphore_wait(barrier, 3)

    mine = pl.ds(core * half, half)
    send_sib = rcopy(h_in, hc.at[1], hsend.at[0], hrecv.at[0], sib)
    send_far = [rcopy(h_in.at[pl.ds(i * half, half), :], hc.at[2 + i, mine, :], hsend.at[1 + i], hrecv.at[1 + i], far) for i in range(2)]
    relay = [rcopy(hc.at[2 + i, mine, :], hc.at[2 + i, mine, :], hsend.at[3 + i], hrecv.at[3 + i], sib) for i in range(2)]
    send_sib.start()
    for c in send_far:
        c.start()
    rcopy(t_in, tg.at[pl.ds(2, 2)], tsend, trecv, sib).start()
    for d in fars:
        for i in range(2):
            rcopy(t_in.at[pl.ds(i, 1)], tg.at[pl.ds(4 + 2 * i + core, 1)], tsend, trecv, d).start()

    zt8[...] = jnp.zeros(zt8.shape, f32)
    ztf[...] = jnp.zeros(ztf.shape, f32)

    def put_stat(pos, v):
        for i in range(2):
            lst[me * 8 + pos * 2 + i] = v[:, i * half:(i + 1) * half]

    def send_stat(pos):
        def go(row, dst_pos, dst_half, d):
            rcopy(lst.at[pl.ds(me * 8 + row, 1)], lst.at[pl.ds(me * 8 + dst_pos * 2 + dst_half, 1)], stsend, strecv.at[dst_pos], d).start()

        near = pos < 2
        for i in range(2):
            go(pos * 2 + i, jnp.where(near, 1 - pos, pos), i, sib)
            for k in range(2):
                go(
                    pos * 2 + i,
                    jnp.where(near, 2 + i, jnp.where(k == i, 0, 1)),
                    jnp.where(near, jnp.where(pos == 0, core, 1 - core), pos - 2),
                    fars[k],
                )

    own_h.wait()
    own_t.wait()
    tg0 = jnp.concatenate([tg[0], tg[1]], axis=1) - base
    put_stat(0, _fwd_chunk(w, hc.at[0], ht.at[0], zb, mb, s8, UN_O, tgt=tg0, zt8=ztf, need=lambda n: wcopy[n].wait(), clear=dw))
    send_stat(0)

    @pl.loop(1, 4)
    def _(pos):
        @pl.when(pos == 1)
        def _():
            send_sib.wait_recv()

        for i in range(2):
            @pl.when(pos == 2 + i)
            def _():
                relay[i].wait_recv()

        def forward():
            for i in range(2):
                @pl.when(pos == 1 + i)
                def _():
                    send_far[i].wait_recv()
                    relay[i].start()

        put_stat(pos, _fwd_chunk(w, hc.at[pos], ht.at[pos], zb, mb, s8, UN_F, mid=forward))
        send_stat(pos)

    wait_bytes(tg.at[pl.ds(2, 6)], trecv)

    def join_stat(pos):
        rows = [[lst[s * 8 + pos * 2 + i] for s in range(4)] for i in range(2)]
        out = []
        for r in rows:
            top = jnp.maximum(jnp.maximum(r[0], r[1]), jnp.maximum(r[2], r[3]))
            out.append(top + jnp.log(sum(jnp.exp(x - top) for x in r)))
        return jnp.concatenate(out, axis=1)

    dpieces = _done_pieces(vloc, UN_B)
    flush = [pltpu.make_async_copy(dw.at[pl.ds(a, n), :], dwp.at[pl.ds(a, n), :], osem.at[i]) for i, (a, n) in enumerate(dpieces)]
    theirs = pl.ds((1 - core) * half, half)
    swap = [rcopy(part.at[i, theirs, :], ring.at[i], psend.at[i], precv.at[i], sib) for i in range(2)]
    cross = [rcopy(part.at[i, mine, :], x_out.at[pl.ds(i * half, half), :], psend.at[2 + i], precv.at[2 + i], far) for i in range(2)]
    last = rcopy(part.at[2], s_out, psend.at[4], precv.at[4], sib)

    lsum = jnp.zeros((1, tok), f32)

    @pl.loop(0, 3)
    def _(i):
        pos = lax.rem(i + 1, 3) + 1
        for q in range(3):
            @pl.when(i == q)
            def _():
                wait_bytes(lst.at[pl.ds(0, 6)], strecv.at[(2, 3, 1)[q]])

        lse = join_stat(pos)
        lsec[pl.ds(pos, 1)] = lse[None]
        tpos = jnp.concatenate([tg[pos * 2], tg[pos * 2 + 1]], axis=1) - base

        def combine():
            for q in range(2):
                @pl.when(i == q + 1)
                def _():
                    swap[q].wait_recv()
                    for j in range(4):
                        rows = pl.ds(core * half + j * (half // 4), half // 4)
                        part[q, rows, :] += ring[q, pl.ds(j * (half // 4), half // 4), :]
                    cross[q].start()

        def done(n, cond):
            pl.when(i == 2 if cond is None else jnp.logical_and(cond, i == 2))(lambda: flush[n].start())

        _bwd_chunk(w, hc.at[pos], ht.at[pos], lse, tpos, dw, dht, zb, gb, UN_B, zt8=zt8, mid=combine, done=done, scale=scale)
        part[i] = dht[...].T
        for q in range(2):
            pl.when(i == q)(lambda q=q: swap[q].start())

    last.start()
    wait_bytes(lst.at[pl.ds(0, 6)], strecv.at[0])
    lsec[0] = join_stat(0)
    lse_out[...] = lsec[0]
    zsum = jnp.sum(zt8[...] + ztf[...], keepdims=True)
    zs[me] = jnp.broadcast_to(zsum, (1, 128))
    for d in [sib] + fars:
        rcopy(zs.at[pl.ds(me, 1)], zs.at[pl.ds(me, 1)], zsend, zrecv, d).start()
    lsum = jnp.sum(lsec[0] + lsec[1] + lsec[2] + lsec[3], keepdims=True)
    wait_bytes(zs.at[pl.ds(0, 3)], zrecv)
    loss_out[...] = (lsum - (zs[0] + zs[1] + zs[2] + zs[3])) * scale
    wait_bytes(zs.at[pl.ds(0, 3)], zsend)
    wait_bytes(lst.at[pl.ds(0, 24)], stsend)
    wait_bytes(tg.at[pl.ds(0, 6)], tsend)
    for c in [send_sib] + send_far + relay + swap:
        c.wait_send()
    for c in flush:
        c.wait()
    for c in cross + [last]:
        c.wait()


def _own_kernel(total, w_in, h_in, t_ref, lse_ref, dwp, x_in, s_in, dwo, dh_ref,
                w, h, ht, xv, sv, dw, dht, z0, z1, g0, g1, wsem, dsem, osem, lsem):
    vloc, depth = w_in.shape
    pieces = _pieces(vloc // SUB, vloc % SUB, UN_L)
    dpieces = _done_pieces(vloc, UN_L)
    wcopy = [pltpu.make_async_copy(w_in.at[pl.ds(a, n), :], w.at[pl.ds(a, n), :], wsem.at[i]) for i, (a, n) in enumerate(pieces)]
    dcopy = [pltpu.make_async_copy(dwp.at[pl.ds(a, n), :], dw.at[pl.ds(a, n), :], dsem.at[i]) for i, (a, n) in enumerate(dpieces)]
    flush = [pltpu.make_async_copy(dw.at[pl.ds(a, n), :], dwo.at[pl.ds(a, n), :], osem.at[i]) for i, (a, n) in enumerate(dpieces)]
    own_h = pltpu.make_async_copy(h_in, h, lsem.at[0])
    recv = [pltpu.make_async_copy(x_in, xv, lsem.at[1]), pltpu.make_async_copy(s_in, sv, lsem.at[2])]
    own_h.start()
    wcopy[0].start()
    for i in range(len(dpieces)):
        wcopy[i + 1].start()
        dcopy[i].start()
    for c in recv:
        c.start()
    own_h.wait()
    ht[...] = h[...].T

    def need(n):
        wcopy[n].wait()
        if n > 0:
            dcopy[n - 1].wait()

    def done(n, cond):
        if cond is None:
            flush[n].start()
        else:
            pl.when(cond)(lambda: flush[n].start())

    tgt = t_ref[...] - lax.axis_index("fsdp") * vloc
    _bwd_chunk(w, h, ht, lse_ref, tgt, dw, dht, (z0, z1), (g0, g1), UN_L, need=need, done=done, scale=1.0 / total)
    for c in recv:
        c.wait()
    dh_ref[...] = dht[...].T + (xv[...] + sv[...])
    for c in flush:
        c.wait()


def solution(mesh):
    groups = mesh.shape["fsdp"]
    tok_spec = P(("dp", "fsdp"), None)

    def local_head(hidden, targets, weight):
        tok, depth = hidden.shape
        vloc = weight.shape[0]
        total = tok * groups
        half = tok // 2
        vm = pltpu.VMEM
        dma = pltpu.SemaphoreType.DMA
        hbm = pl.BlockSpec(memory_space=pl.ANY)
        loc = pl.BlockSpec(memory_space=pltpu.VMEM)
        np_f = len(_pieces(vloc // SUB, vloc % SUB, UN_O))
        np_b = len(_pieces(vloc // SUB, vloc % SUB, UN_L))
        nd = len(_done_pieces(vloc, UN_B))
        nl = len(_done_pieces(vloc, UN_L))
        sds = jax.ShapeDtypeStruct
        dwp, x, s, lse, loss = pl.pallas_call(
            lambda *refs: _exchange_kernel(total, *refs),
            in_specs=[hbm, hbm, hbm],
            out_specs=[hbm, hbm, hbm, loc, loc],
            out_shape=[sds((vloc, depth), f32), sds((tok, depth), f32), sds((tok, depth), f32), sds((1, tok), f32), sds((1, 128), f32)],
            scratch_shapes=[
                vm((vloc, depth), bf16), vm((groups, tok, depth), bf16), vm((groups, depth, tok), bf16), vm((vloc, depth), f32),
                vm((depth, tok), f32), vm((3, tok, depth), f32), vm((2, half, depth), f32),
                vm((8, 1, half), jnp.int32), vm((32, 1, half), f32), vm((4, 1, 128), f32), vm((4, 1, tok), f32),
                vm((SUB, tok), f32), vm((SUB, tok), f32), vm((SUB, tok), bf16), vm((SUB, tok), bf16),
                vm((8, tok), f32), vm((8, tok), f32), vm((8, tok), f32), vm((8, tok), f32), vm((8, tok), f32), vm((8, tok), f32),
                dma((np_f,)), dma((2,)), dma((5,)), dma((5,)), dma, dma, dma, dma((4,)), dma((5,)), dma((5,)), dma, dma, dma((nd,)),
            ],
            compiler_params=pltpu.CompilerParams(vmem_limit_bytes=66_500_000, collective_id=0, has_side_effects=True),
            name="ce_exchange",
        )(hidden, targets.reshape(2, 1, half), weight)
        dw, dh = pl.pallas_call(
            lambda *refs: _own_kernel(total, *refs),
            in_specs=[hbm, hbm, loc, loc, hbm, hbm, hbm],
            out_specs=[hbm, loc],
            out_shape=[sds((vloc, depth), f32), sds((tok, depth), f32)],
            scratch_shapes=[
                vm((vloc, depth), bf16), vm((tok, depth), bf16), vm((depth, tok), bf16), vm((tok, depth), f32), vm((tok, depth), f32),
                vm((vloc, depth), f32), vm((depth, tok), f32),
                vm((SUB, tok), f32), vm((SUB, tok), f32), vm((SUB, tok), bf16), vm((SUB, tok), bf16),
                dma((np_b,)), dma((nl,)), dma((nl,)), dma((3,)),
            ],
            compiler_params=pltpu.CompilerParams(vmem_limit_bytes=66_500_000),
            name="ce_own",
        )(weight, hidden, targets[None, :], lse, dwp, x, s)
        return loss[0, :1], dh, dw

    return jax.shard_map(local_head, mesh=mesh, in_specs=(tok_spec, P(("dp", "fsdp")), P("fsdp", None)), out_specs=(P("dp"), tok_spec, tok_spec), check_vma=False)
```

```python
import jax
import jax.numpy as jnp
from jax import lax
from jax.experimental import pallas as pl
from jax.experimental.pallas import tpu as pltpu
from jax.sharding import PartitionSpec as P

SUB = 256
UN_O = 4
UN_F = 14
UN_B = 14
UN_L = 4
VMEM_X = 44_000_000
VMEM_L = 30_000_000
f32 = jnp.float32
bf16 = jnp.bfloat16
MESH = pl.DeviceIdType.MESH


def _nn(a, b):
    return lax.dot_general(a, b, (((1,), (0,)), ((), ())), preferred_element_type=f32)


def _tn(a, b):
    return lax.dot_general(a, b, (((0,), (0,)), ((), ())), preferred_element_type=f32)


def _pieces(full, rem, unroll):
    loops = (full - 2) // unroll
    cuts = [0, 2 * SUB] + [(2 + (i + 1) * unroll) * SUB for i in range(loops)] + [full * SUB + rem]
    return [(a, b - a) for a, b in zip(cuts[:-1], cuts[1:])]


def _fwd_chunk(w, h, ht, zb, mb, s8, un, tgt=None, zt8=None, mid=None, need=None, clear=None):
    vloc = w.shape[0]
    tok = h.shape[0]
    full, rem = vloc // SUB, vloc % SUB
    loops = (full - 2) // un
    ht[...] = h[...].T
    mb[1][...] = jnp.full(mb[1].shape, -jnp.inf, f32)
    s8[...] = jnp.zeros(s8.shape, f32)

    def zdot(k, slot, rows=SUB):
        z = _nn(w[pl.ds(k * SUB, rows), :], ht[...])
        zb[slot][pl.ds(0, rows), :] = z
        mb[slot][...] = jnp.maximum(mb[1 - slot][...], jnp.max(z.reshape(rows // 8, 8, tok), axis=0))

    def epi(k, slot, rows=SUB):
        z = zb[slot][pl.ds(0, rows), :].reshape(rows // 8, 8, tok)
        new = mb[slot][...]
        s8[...] = s8[...] * jnp.exp(mb[2][...] - new) + jnp.sum(jnp.exp(z - new[None]), axis=0)
        mb[2][...] = new
        if clear is not None:
            clear[pl.ds(k * SUB, rows), :] = jnp.zeros((rows, clear.shape[1]), f32)
        if tgt is not None:
            t = tgt - k * SUB
            lane = lax.broadcasted_iota(jnp.int32, (8, tok), 0)
            acc = zt8[...]
            for r in range(rows // 8):
                acc = jnp.where(lane + r * 8 == t, z[r], acc)
            zt8[...] = acc

    def step(k, par, zrows=SUB, erows=SUB):
        if zrows:
            zdot(k + 1, 1 - par, zrows)
        if erows:
            epi(k, par, erows)

    mb[2][...] = mb[1][...]
    if need is not None:
        need(0)
    zdot(0, 0)
    step(0, 0)

    @pl.loop(0, loops)
    def _(i):
        if need is not None:
            for n in range(loops):
                pl.when(i == n)(lambda n=n: need(1 + n))
        for u in range(un):
            step(1 + i * un + u, (1 + u) % 2)
        if mid is not None:
            pl.when(i == 0)(mid)

    if need is not None:
        need(1 + loops)
    for k in range(1 + loops * un, full - 1):
        step(k, k % 2)
    step(full - 1, (full - 1) % 2, zrows=rem)
    step(full, full % 2, zrows=0, erows=rem)
    m8 = mb[2][...]
    top = jnp.max(m8, axis=0, keepdims=True)
    return top + jnp.log(jnp.sum(s8[...] * jnp.exp(m8 - top), axis=0, keepdims=True))


def _bwd_chunk(w, h, ht, lse, tgt, dw, dht, zb, gb, un, zt8=None, mid=None, need=None, done=None, scale=1.0):
    vloc = w.shape[0]
    tok = h.shape[0]
    full, rem = vloc // SUB, vloc % SUB
    loops = (full - 2) // un

    def zdot(k, slot, rows=SUB):
        zb[slot][pl.ds(0, rows), :] = _nn(w[pl.ds(k * SUB, rows), :], ht[...])

    def epi(k, slot, rows=SUB):
        z = zb[slot][pl.ds(0, rows), :]
        hit = lax.broadcasted_iota(jnp.int32, (rows, tok), 0) == tgt[...] - k * SUB
        p = jnp.exp(z - lse[...])
        if zt8 is not None:
            zt8[...] += jnp.sum(jnp.where(hit, z, 0.0).reshape(rows // 8, 8, tok), axis=0)
        gb[slot][pl.ds(0, rows), :] = ((p - jnp.where(hit, 1.0, 0.0)) * scale).astype(bf16)

    def ddot(k, slot, rows=SUB):
        g = gb[slot][pl.ds(0, rows), :]
        rng = pl.ds(k * SUB, rows)
        dw[rng, :] = dw[rng, :] + _nn(g, h[...])
        dht[...] += _tn(w[rng, :], g)

    def step(k, par, zrows=SUB, erows=SUB, drows=SUB):
        if drows:
            ddot(k - 1, 1 - par, drows)
        if zrows:
            zdot(k + 1, 1 - par, zrows)
        if erows:
            epi(k, par, erows)

    dht[...] = jnp.zeros(dht.shape, f32)
    if need is not None:
        need(0)
    zdot(0, 0)
    step(0, 0, drows=0)
    if mid is not None:
        mid()

    @pl.loop(0, loops)
    def _(i):
        if need is not None:
            for n in range(loops):
                pl.when(i == n)(lambda n=n: need(1 + n))
        for u in range(un):
            step(1 + i * un + u, (1 + u) % 2)
        if done is not None:
            for n in range(loops):
                done(n, i == n)

    if need is not None:
        need(1 + loops)
    for k in range(1 + loops * un, full - 1):
        step(k, k % 2)
    step(full - 1, (full - 1) % 2, zrows=rem)
    step(full, full % 2, zrows=0, erows=rem)
    step(full + 1, (full + 1) % 2, zrows=0, erows=0, drows=rem)
    if done is not None:
        done(loops, None)


def _done_pieces(vloc, un):
    full = vloc // SUB
    loops = (full - 2) // un
    cuts = [0] + [(i + 1) * un * SUB for i in range(loops)] + [vloc]
    return [(a, b - a) for a, b in zip(cuts[:-1], cuts[1:])]


def _exchange_kernel(total, h_in, t_in, w_in, dwp, w, h0, x_out, s_out, lse_out, loss_out,
                     dw, hc, ht0, ht, dht, part, ring, tg, lst, zs, lsec, z0, z1, g0, g1, ma, mb_, mc, s8, zt8, ztf,
                     wsem, lsem, hsend, hrecv, tsend, trecv, stsend, strecv, psend, precv, zsend, zrecv, osem):
    vloc, depth = w_in.shape
    tok = h_in.shape[0]
    half = tok // 2
    me = lax.axis_index("fsdp")
    chip, core = me // 2, me % 2
    sib = 2 * chip + (1 - core)
    far = 2 * (1 - chip) + core
    fars = [2 * (1 - chip), 2 * (1 - chip) + 1]
    base = me * vloc
    dev = lambda d: {"fsdp": d}
    zb, gb, mb = (z0, z1), (g0, g1), (ma, mb_, mc)
    scale = 1.0 / total

    def rcopy(src, dst, ssem, rsem, d):
        return pltpu.make_async_remote_copy(src_ref=src, dst_ref=dst, send_sem=ssem, recv_sem=rsem, device_id=dev(d), device_id_type=MESH)

    def wait_bytes(ref, sem):
        pltpu.make_async_copy(ref, ref, sem).wait()

    pieces = _pieces(vloc // SUB, vloc % SUB, UN_O)
    wcopy = [pltpu.make_async_copy(w_in.at[pl.ds(a, n), :], w.at[pl.ds(a, n), :], wsem.at[i]) for i, (a, n) in enumerate(pieces)]
    own_h = pltpu.make_async_copy(h_in, h0, lsem.at[0])
    own_t = pltpu.make_async_copy(t_in, tg.at[pl.ds(0, 2)], lsem.at[1])
    own_h.start()
    own_t.start()
    for c in wcopy:
        c.start()

    barrier = pltpu.get_barrier_semaphore()
    for d in [sib] + fars:
        pl.semaphore_signal(barrier, inc=1, device_id=dev(d), device_id_type=MESH)
    pl.semaphore_wait(barrier, 3)

    mine = pl.ds(core * half, half)
    send_sib = rcopy(h_in, hc.at[0], hsend.at[0], hrecv.at[0], sib)
    send_far = [rcopy(h_in.at[pl.ds(i * half, half), :], hc.at[1 + i, mine, :], hsend.at[1 + i], hrecv.at[1 + i], far) for i in range(2)]
    relay = [rcopy(hc.at[1 + i, mine, :], hc.at[1 + i, mine, :], hsend.at[3 + i], hrecv.at[3 + i], sib) for i in range(2)]
    send_sib.start()
    for c in send_far:
        c.start()
    rcopy(t_in, tg.at[pl.ds(2, 2)], tsend, trecv, sib).start()
    for d in fars:
        for i in range(2):
            rcopy(t_in.at[pl.ds(i, 1)], tg.at[pl.ds(4 + 2 * i + core, 1)], tsend, trecv, d).start()

    zt8[...] = jnp.zeros(zt8.shape, f32)
    ztf[...] = jnp.zeros(ztf.shape, f32)

    def put_stat(pos, v):
        for i in range(2):
            lst[me * 8 + pos * 2 + i] = v[:, i * half:(i + 1) * half]

    def send_stat(pos):
        def go(row, dst_pos, dst_half, d):
            rcopy(lst.at[pl.ds(me * 8 + row, 1)], lst.at[pl.ds(me * 8 + dst_pos * 2 + dst_half, 1)], stsend, strecv.at[dst_pos], d).start()

        near = pos < 2
        for i in range(2):
            go(pos * 2 + i, jnp.where(near, 1 - pos, pos), i, sib)
            for k in range(2):
                go(
                    pos * 2 + i,
                    jnp.where(near, 2 + i, jnp.where(k == i, 0, 1)),
                    jnp.where(near, jnp.where(pos == 0, core, 1 - core), pos - 2),
                    fars[k],
                )

    own_h.wait()
    own_t.wait()
    tg0 = jnp.concatenate([tg[0], tg[1]], axis=1) - base
    put_stat(0, _fwd_chunk(w, h0, ht0, zb, mb, s8, UN_O, tgt=tg0, zt8=ztf, need=lambda n: wcopy[n].wait(), clear=dw))
    send_stat(0)

    @pl.loop(1, 4)
    def _(pos):
        @pl.when(pos == 1)
        def _():
            send_sib.wait_recv()

        for i in range(2):
            @pl.when(pos == 2 + i)
            def _():
                relay[i].wait_recv()

        def forward():
            for i in range(2):
                @pl.when(pos == 1 + i)
                def _():
                    send_far[i].wait_recv()
                    relay[i].start()

        put_stat(pos, _fwd_chunk(w, hc.at[pos - 1], ht.at[pos - 1], zb, mb, s8, UN_F, mid=forward))
        send_stat(pos)

    wait_bytes(tg.at[pl.ds(2, 6)], trecv)

    def join_stat(pos):
        rows = [[lst[s * 8 + pos * 2 + i] for s in range(4)] for i in range(2)]
        out = []
        for r in rows:
            top = jnp.maximum(jnp.maximum(r[0], r[1]), jnp.maximum(r[2], r[3]))
            out.append(top + jnp.log(sum(jnp.exp(x - top) for x in r)))
        return jnp.concatenate(out, axis=1)

    dpieces = _done_pieces(vloc, UN_B)
    flush = [pltpu.make_async_copy(dw.at[pl.ds(a, n), :], dwp.at[pl.ds(a, n), :], osem.at[i]) for i, (a, n) in enumerate(dpieces)]
    theirs = pl.ds((1 - core) * half, half)
    swap = [rcopy(part.at[i, theirs, :], ring.at[i], psend.at[i], precv.at[i], sib) for i in range(2)]
    cross = [rcopy(part.at[i, mine, :], x_out.at[pl.ds(i * half, half), :], psend.at[2 + i], precv.at[2 + i], far) for i in range(2)]
    last = rcopy(part.at[2], s_out, psend.at[4], precv.at[4], sib)

    lsum = jnp.zeros((1, tok), f32)

    @pl.loop(0, 3)
    def _(i):
        pos = lax.rem(i + 1, 3) + 1
        for q in range(3):
            @pl.when(i == q)
            def _():
                wait_bytes(lst.at[pl.ds(0, 6)], strecv.at[(2, 3, 1)[q]])

        lse = join_stat(pos)
        lsec[pl.ds(pos, 1)] = lse[None]
        tpos = jnp.concatenate([tg[pos * 2], tg[pos * 2 + 1]], axis=1) - base

        def combine():
            for q in range(2):
                @pl.when(i == q + 1)
                def _():
                    swap[q].wait_recv()
                    for j in range(4):
                        rows = pl.ds(core * half + j * (half // 4), half // 4)
                        part[q, rows, :] += ring[q, pl.ds(j * (half // 4), half // 4), :]
                    cross[q].start()

        def done(n, cond):
            pl.when(i == 2 if cond is None else jnp.logical_and(cond, i == 2))(lambda: flush[n].start())

        _bwd_chunk(w, hc.at[pos - 1], ht.at[pos - 1], lse, tpos, dw, dht, zb, gb, UN_B, zt8=zt8, mid=combine, done=done, scale=scale)
        part[i] = dht[...].T
        for q in range(2):
            pl.when(i == q)(lambda q=q: swap[q].start())

    last.start()
    wait_bytes(lst.at[pl.ds(0, 6)], strecv.at[0])
    lsec[0] = join_stat(0)
    lse_out[...] = lsec[0]
    zsum = jnp.sum(zt8[...] + ztf[...], keepdims=True)
    zs[me] = jnp.broadcast_to(zsum, (1, 128))
    for d in [sib] + fars:
        rcopy(zs.at[pl.ds(me, 1)], zs.at[pl.ds(me, 1)], zsend, zrecv, d).start()
    lsum = jnp.sum(lsec[0] + lsec[1] + lsec[2] + lsec[3], keepdims=True)
    wait_bytes(zs.at[pl.ds(0, 3)], zrecv)
    loss_out[...] = (lsum - (zs[0] + zs[1] + zs[2] + zs[3])) * scale
    wait_bytes(zs.at[pl.ds(0, 3)], zsend)
    wait_bytes(lst.at[pl.ds(0, 24)], stsend)
    wait_bytes(tg.at[pl.ds(0, 6)], tsend)
    for c in [send_sib] + send_far + relay + swap:
        c.wait_send()
    for c in flush:
        c.wait()
    for c in cross + [last]:
        c.wait()


def _own_kernel(total, dwp, w, h, x, s, t_ref, lse_ref, dwo, dh_ref, dw, ht, dht, z0, z1, g0, g1, dsem, osem):
    vloc = w.shape[0]
    dpieces = _done_pieces(vloc, UN_L)
    dcopy = [pltpu.make_async_copy(dwp.at[pl.ds(a, n), :], dw.at[pl.ds(a, n), :], dsem.at[i]) for i, (a, n) in enumerate(dpieces)]
    flush = [pltpu.make_async_copy(dw.at[pl.ds(a, n), :], dwo.at[pl.ds(a, n), :], osem.at[i]) for i, (a, n) in enumerate(dpieces)]

    def done(n, cond):
        if cond is None:
            flush[n].start()
        else:
            pl.when(cond)(lambda: flush[n].start())

    for c in dcopy:
        c.start()
    ht[...] = h[...].T

    def need(n):
        if n > 0:
            dcopy[n - 1].wait()

    tgt = t_ref[...] - lax.axis_index("fsdp") * vloc
    _bwd_chunk(w, h, ht, lse_ref, tgt, dw, dht, (z0, z1), (g0, g1), UN_L, need=need, done=done, scale=1.0 / total)
    dh_ref[...] = dht[...].T + (x[...] + s[...])
    for c in flush:
        c.wait()


def solution(mesh):
    groups = mesh.shape["fsdp"]
    tok_spec = P(("dp", "fsdp"), None)

    def local_head(hidden, targets, weight):
        tok, depth = hidden.shape
        vloc = weight.shape[0]
        total = tok * groups
        half = tok // 2
        vm = pltpu.VMEM
        dma = pltpu.SemaphoreType.DMA
        hbm = pl.BlockSpec(memory_space=pl.ANY)
        loc = pl.BlockSpec(memory_space=pltpu.VMEM)
        np_f = len(_pieces(vloc // SUB, vloc % SUB, UN_O))
        nl = len(_done_pieces(vloc, UN_L))
        sds = jax.ShapeDtypeStruct
        work = [vm((SUB, tok), f32), vm((SUB, tok), f32), vm((SUB, tok), bf16), vm((SUB, tok), bf16)]
        nd = len(_done_pieces(vloc, UN_B))
        dwp, w, h0, x, s, lse, loss = pl.pallas_call(
            lambda *refs: _exchange_kernel(total, *refs),
            in_specs=[hbm, hbm, hbm],
            out_specs=[hbm] + [loc] * 6,
            out_shape=[
                sds((vloc, depth), f32), vm((vloc, depth), bf16), vm((tok, depth), bf16),
                vm((tok, depth), f32), vm((tok, depth), f32), vm((1, tok), f32), sds((1, 128), f32),
            ],
            scratch_shapes=[
                vm((vloc, depth), f32), vm((groups - 1, tok, depth), bf16), vm((depth, tok), bf16), vm((groups - 1, depth, tok), bf16),
                vm((depth, tok), f32), vm((3, tok, depth), f32), vm((2, half, depth), f32),
                vm((8, 1, half), jnp.int32), vm((32, 1, half), f32), vm((4, 1, 128), f32), vm((4, 1, tok), f32),
            ] + work + [vm((8, tok), f32)] * 6 + [
                dma((np_f,)), dma((2,)), dma((5,)), dma((5,)), dma, dma, dma, dma((4,)), dma((5,)), dma((5,)), dma, dma, dma((nd,)),
            ],
            compiler_params=pltpu.CompilerParams(vmem_limit_bytes=VMEM_X, collective_id=0, has_side_effects=True),
            name="ce_exchange",
        )(hidden, targets.reshape(2, 1, half), weight)
        keep = lambda a: pltpu.with_memory_space_constraint(a, pltpu.VMEM)
        grad_w, dh = pl.pallas_call(
            lambda *refs: _own_kernel(total, *refs),
            in_specs=[hbm] + [loc] * 6,
            out_specs=[hbm, loc],
            out_shape=[sds((vloc, depth), f32), sds((tok, depth), f32)],
            scratch_shapes=[vm((vloc, depth), f32), vm((depth, tok), bf16), vm((depth, tok), f32)] + work + [dma((nl,)), dma((nl,))],
            compiler_params=pltpu.CompilerParams(vmem_limit_bytes=VMEM_L),
            name="ce_own",
        )(dwp, *[keep(a) for a in (w, h0, x, s)], targets[None, :], keep(lse))
        return loss[0, :1], dh, grad_w

    return jax.shard_map(local_head, mesh=mesh, in_specs=(tok_spec, P(("dp", "fsdp")), P("fsdp", None)), out_specs=(P("dp"), tok_spec, tok_spec), check_vma=False)
```

```python
import jax
import jax.numpy as jnp
from jax import lax
from jax.experimental import pallas as pl
from jax.experimental.pallas import tpu as pltpu
from jax.sharding import PartitionSpec as P

SUB = 256
UN_O = 4
UN_F = 14
UN_B = 14
UN_L = 4
VMEM_X = 56_500_000
VMEM_L = 56_500_000
f32 = jnp.float32
bf16 = jnp.bfloat16
MESH = pl.DeviceIdType.MESH


def _nn(a, b):
    return lax.dot_general(a, b, (((1,), (0,)), ((), ())), preferred_element_type=f32)


def _tn(a, b):
    return lax.dot_general(a, b, (((0,), (0,)), ((), ())), preferred_element_type=f32)


def _pieces(full, rem, unroll):
    loops = (full - 2) // unroll
    cuts = [0, 2 * SUB] + [(2 + (i + 1) * unroll) * SUB for i in range(loops)] + [full * SUB + rem]
    return [(a, b - a) for a, b in zip(cuts[:-1], cuts[1:])]


def _fwd_chunk(w, h, ht, zb, mb, s8, un, tgt=None, zt8=None, mid=None, need=None, clear=None):
    vloc = w.shape[0]
    tok = h.shape[0]
    full, rem = vloc // SUB, vloc % SUB
    loops = (full - 2) // un
    ht[...] = h[...].T
    mb[1][...] = jnp.full(mb[1].shape, -jnp.inf, f32)
    s8[...] = jnp.zeros(s8.shape, f32)

    def zdot(k, slot, rows=SUB):
        z = _nn(w[pl.ds(k * SUB, rows), :], ht[...])
        zb[slot][pl.ds(0, rows), :] = z
        mb[slot][...] = jnp.maximum(mb[1 - slot][...], jnp.max(z.reshape(rows // 8, 8, tok), axis=0))

    def epi(k, slot, rows=SUB):
        z = zb[slot][pl.ds(0, rows), :].reshape(rows // 8, 8, tok)
        new = mb[slot][...]
        s8[...] = s8[...] * jnp.exp(mb[2][...] - new) + jnp.sum(jnp.exp(z - new[None]), axis=0)
        mb[2][...] = new
        if clear is not None:
            clear[pl.ds(k * SUB, rows), :] = jnp.zeros((rows, clear.shape[1]), f32)
        if tgt is not None:
            t = tgt - k * SUB
            lane = lax.broadcasted_iota(jnp.int32, (8, tok), 0)
            acc = zt8[...]
            for r in range(rows // 8):
                acc = jnp.where(lane + r * 8 == t, z[r], acc)
            zt8[...] = acc

    def step(k, par, zrows=SUB, erows=SUB):
        if zrows:
            zdot(k + 1, 1 - par, zrows)
        if erows:
            epi(k, par, erows)

    mb[2][...] = mb[1][...]
    if need is not None:
        need(0)
    zdot(0, 0)
    step(0, 0)

    @pl.loop(0, loops)
    def _(i):
        if need is not None:
            for n in range(loops):
                pl.when(i == n)(lambda n=n: need(1 + n))
        for u in range(un):
            step(1 + i * un + u, (1 + u) % 2)
        if mid is not None:
            pl.when(i == 0)(mid)

    if need is not None:
        need(1 + loops)
    for k in range(1 + loops * un, full - 1):
        step(k, k % 2)
    step(full - 1, (full - 1) % 2, zrows=rem)
    step(full, full % 2, zrows=0, erows=rem)
    m8 = mb[2][...]
    top = jnp.max(m8, axis=0, keepdims=True)
    return top + jnp.log(jnp.sum(s8[...] * jnp.exp(m8 - top), axis=0, keepdims=True))


def _bwd_chunk(w, h, ht, lse, tgt, dw, dht, zb, gb, un, zt8=None, mid=None, late=None, need=None, done=None, scale=1.0):
    vloc = w.shape[0]
    tok = h.shape[0]
    full, rem = vloc // SUB, vloc % SUB
    loops = (full - 2) // un

    def zdot(k, slot, rows=SUB):
        zb[slot][pl.ds(0, rows), :] = _nn(w[pl.ds(k * SUB, rows), :], ht[...])

    def epi(k, slot, rows=SUB):
        z = zb[slot][pl.ds(0, rows), :]
        hit = lax.broadcasted_iota(jnp.int32, (rows, tok), 0) == tgt[...] - k * SUB
        p = jnp.exp(z - lse[...])
        if zt8 is not None:
            zt8[...] += jnp.sum(jnp.where(hit, z, 0.0).reshape(rows // 8, 8, tok), axis=0)
        gb[slot][pl.ds(0, rows), :] = ((p - jnp.where(hit, 1.0, 0.0)) * scale).astype(bf16)

    def ddot(k, slot, rows=SUB):
        g = gb[slot][pl.ds(0, rows), :]
        rng = pl.ds(k * SUB, rows)
        dw[rng, :] = dw[rng, :] + _nn(g, h[...])
        dht[...] += _tn(w[rng, :], g)

    def step(k, par, zrows=SUB, erows=SUB, drows=SUB):
        if drows:
            ddot(k - 1, 1 - par, drows)
        if zrows:
            zdot(k + 1, 1 - par, zrows)
        if erows:
            epi(k, par, erows)

    dht[...] = jnp.zeros(dht.shape, f32)
    if need is not None:
        need(0)
    zdot(0, 0)
    step(0, 0, drows=0)
    if mid is not None:
        mid()

    @pl.loop(0, loops)
    def _(i):
        if need is not None:
            for n in range(loops):
                pl.when(i == n)(lambda n=n: need(1 + n))
        for u in range(un):
            step(1 + i * un + u, (1 + u) % 2)
        if late is not None:
            pl.when(i == 0)(late)
        if done is not None:
            for n in range(loops):
                done(n, i == n)

    if need is not None:
        need(1 + loops)
    for k in range(1 + loops * un, full - 1):
        step(k, k % 2)
    step(full - 1, (full - 1) % 2, zrows=rem)
    step(full, full % 2, zrows=0, erows=rem)
    step(full + 1, (full + 1) % 2, zrows=0, erows=0, drows=rem)
    if done is not None:
        done(loops, None)


def _done_pieces(vloc, un):
    full = vloc // SUB
    loops = (full - 2) // un
    cuts = [0] + [(i + 1) * un * SUB for i in range(loops)] + [vloc]
    return [(a, b - a) for a, b in zip(cuts[:-1], cuts[1:])]


def _exchange_kernel(total, h_in, t_in, w_in, dwp, w, h0, x_out, s_out, lse_out, loss_out,
                     dw, hc, ht0, ht, dht, part, ring, tg, lst, zs, lsec, z0, z1, g0, g1, ma, mb_, mc, s8, zt8, ztf,
                     wsem, lsem, hsend, hrecv, tsend, trecv, stsend, strecv, psend, precv, zsend, zrecv, osem):
    vloc, depth = w_in.shape
    tok = h_in.shape[0]
    half = tok // 2
    me = lax.axis_index("fsdp")
    chip, core = me // 2, me % 2
    sib = 2 * chip + (1 - core)
    far = 2 * (1 - chip) + core
    fars = [2 * (1 - chip), 2 * (1 - chip) + 1]
    base = me * vloc
    dev = lambda d: {"fsdp": d}
    zb, gb, mb = (z0, z1), (g0, g1), (ma, mb_, mc)
    scale = 1.0 / total

    def rcopy(src, dst, ssem, rsem, d):
        return pltpu.make_async_remote_copy(src_ref=src, dst_ref=dst, send_sem=ssem, recv_sem=rsem, device_id=dev(d), device_id_type=MESH)

    def wait_bytes(ref, sem):
        pltpu.make_async_copy(ref, ref, sem).wait()

    pieces = _pieces(vloc // SUB, vloc % SUB, UN_O)
    wcopy = [pltpu.make_async_copy(w_in.at[pl.ds(a, n), :], w.at[pl.ds(a, n), :], wsem.at[i]) for i, (a, n) in enumerate(pieces)]
    own_h = pltpu.make_async_copy(h_in, h0, lsem.at[0])
    own_t = pltpu.make_async_copy(t_in, tg.at[pl.ds(0, 2)], lsem.at[1])
    own_h.start()
    own_t.start()
    for c in wcopy:
        c.start()

    barrier = pltpu.get_barrier_semaphore()
    for d in [sib] + fars:
        pl.semaphore_signal(barrier, inc=1, device_id=dev(d), device_id_type=MESH)
    pl.semaphore_wait(barrier, 3)

    mine = pl.ds(core * half, half)
    send_sib = rcopy(h_in, hc.at[0], hsend.at[0], hrecv.at[0], sib)
    send_far = [rcopy(h_in.at[pl.ds(i * half, half), :], hc.at[1 + i, mine, :], hsend.at[1 + i], hrecv.at[1 + i], far) for i in range(2)]
    relay = [rcopy(hc.at[1 + i, mine, :], hc.at[1 + i, mine, :], hsend.at[3 + i], hrecv.at[3 + i], sib) for i in range(2)]
    send_sib.start()
    for c in send_far:
        c.start()
    rcopy(t_in, tg.at[pl.ds(2, 2)], tsend, trecv, sib).start()
    for d in fars:
        for i in range(2):
            rcopy(t_in.at[pl.ds(i, 1)], tg.at[pl.ds(4 + 2 * i + core, 1)], tsend, trecv, d).start()

    zt8[...] = jnp.zeros(zt8.shape, f32)
    ztf[...] = jnp.zeros(ztf.shape, f32)

    def put_stat(pos, v):
        for i in range(2):
            lst[me * 8 + pos * 2 + i] = v[:, i * half:(i + 1) * half]

    def send_stat(pos):
        def go(row, dst_pos, dst_half, d):
            rcopy(lst.at[pl.ds(me * 8 + row, 1)], lst.at[pl.ds(me * 8 + dst_pos * 2 + dst_half, 1)], stsend, strecv.at[dst_pos], d).start()

        near = pos < 2
        for i in range(2):
            go(pos * 2 + i, jnp.where(near, 1 - pos, pos), i, sib)
            for k in range(2):
                go(
                    pos * 2 + i,
                    jnp.where(near, 2 + i, jnp.where(k == i, 0, 1)),
                    jnp.where(near, jnp.where(pos == 0, core, 1 - core), pos - 2),
                    fars[k],
                )

    own_h.wait()
    own_t.wait()
    tg0 = jnp.concatenate([tg[0], tg[1]], axis=1) - base
    put_stat(0, _fwd_chunk(w, h0, ht0, zb, mb, s8, UN_O, tgt=tg0, zt8=ztf, need=lambda n: wcopy[n].wait(), clear=dw))
    send_stat(0)

    @pl.loop(1, 4)
    def _(pos):
        @pl.when(pos == 1)
        def _():
            send_sib.wait_recv()

        for i in range(2):
            @pl.when(pos == 2 + i)
            def _():
                relay[i].wait_recv()

        def forward():
            for i in range(2):
                @pl.when(pos == 1 + i)
                def _():
                    send_far[i].wait_recv()
                    relay[i].start()

        put_stat(pos, _fwd_chunk(w, hc.at[pos - 1], ht.at[pos - 1], zb, mb, s8, UN_F, mid=forward))
        send_stat(pos)

    wait_bytes(tg.at[pl.ds(2, 6)], trecv)

    def join_stat(pos):
        rows = [[lst[s * 8 + pos * 2 + i] for s in range(4)] for i in range(2)]
        out = []
        for r in rows:
            top = jnp.maximum(jnp.maximum(r[0], r[1]), jnp.maximum(r[2], r[3]))
            out.append(top + jnp.log(sum(jnp.exp(x - top) for x in r)))
        return jnp.concatenate(out, axis=1)

    dpieces = _done_pieces(vloc, UN_B)
    flush = [pltpu.make_async_copy(dw.at[pl.ds(a, n), :], dwp.at[pl.ds(a, n), :], osem.at[i]) for i, (a, n) in enumerate(dpieces)]
    theirs = pl.ds((1 - core) * half, half)
    swap = [rcopy(part.at[i, theirs, :], ring.at[i], psend.at[i], precv.at[i], sib) for i in range(2)]
    cross = [rcopy(part.at[i, mine, :], x_out.at[pl.ds(i * half, half), :], psend.at[2 + i], precv.at[2 + i], far) for i in range(2)]
    last = rcopy(part.at[2], s_out, psend.at[4], precv.at[4], sib)

    lsum = jnp.zeros((1, tok), f32)

    @pl.loop(0, 3)
    def _(i):
        pos = lax.rem(i + 1, 3) + 1
        for q in range(3):
            @pl.when(i == q)
            def _():
                wait_bytes(lst.at[pl.ds(0, 6)], strecv.at[(2, 3, 1)[q]])

        lse = join_stat(pos)
        lsec[pl.ds(pos, 1)] = lse[None]
        tpos = jnp.concatenate([tg[pos * 2], tg[pos * 2 + 1]], axis=1) - base

        def combine(q):
            @pl.when(i == q + 1)
            def _():
                swap[q].wait_recv()
                for j in range(4):
                    rows = pl.ds(core * half + j * (half // 4), half // 4)
                    part[q, rows, :] += ring[q, pl.ds(j * (half // 4), half // 4), :]
                cross[q].start()

        def done(n, cond):
            pl.when(i == 2 if cond is None else jnp.logical_and(cond, i == 2))(lambda: flush[n].start())

        _bwd_chunk(w, hc.at[pos - 1], ht.at[pos - 1], lse, tpos, dw, dht, zb, gb, UN_B, zt8=zt8, mid=lambda: combine(1), late=lambda: combine(0), done=done, scale=scale)
        part[i] = dht[...].T
        for q in range(2):
            pl.when(i == q)(lambda q=q: swap[q].start())

    last.start()
    wait_bytes(lst.at[pl.ds(0, 6)], strecv.at[0])
    lsec[0] = join_stat(0)
    lse_out[...] = lsec[0]
    zsum = jnp.sum(zt8[...] + ztf[...], keepdims=True)
    zs[me] = jnp.broadcast_to(zsum, (1, 128))
    for d in [sib] + fars:
        rcopy(zs.at[pl.ds(me, 1)], zs.at[pl.ds(me, 1)], zsend, zrecv, d).start()
    lsum = jnp.sum(lsec[0] + lsec[1] + lsec[2] + lsec[3], keepdims=True)
    wait_bytes(zs.at[pl.ds(0, 3)], zrecv)
    loss_out[...] = (lsum - (zs[0] + zs[1] + zs[2] + zs[3])) * scale
    wait_bytes(zs.at[pl.ds(0, 3)], zsend)
    wait_bytes(lst.at[pl.ds(0, 24)], stsend)
    wait_bytes(tg.at[pl.ds(0, 6)], tsend)
    for c in [send_sib] + send_far + relay + swap:
        c.wait_send()
    for c in flush:
        c.wait()
    for c in cross + [last]:
        c.wait()


def _own_kernel(total, dwp, w, h, x_in, s_in, t_ref, lse_ref, dwo, dh_ref, dw, x, s, ht, dht, z0, z1, g0, g1, dsem, osem, lsem):
    vloc = w.shape[0]
    dpieces = _done_pieces(vloc, UN_L)
    dcopy = [pltpu.make_async_copy(dwp.at[pl.ds(a, n), :], dw.at[pl.ds(a, n), :], dsem.at[i]) for i, (a, n) in enumerate(dpieces)]
    flush = [pltpu.make_async_copy(dw.at[pl.ds(a, n), :], dwo.at[pl.ds(a, n), :], osem.at[i]) for i, (a, n) in enumerate(dpieces)]

    def done(n, cond):
        if cond is None:
            flush[n].start()
        else:
            pl.when(cond)(lambda: flush[n].start())

    recv = [pltpu.make_async_copy(x_in, x, lsem.at[0]), pltpu.make_async_copy(s_in, s, lsem.at[1])]
    for c in dcopy + recv:
        c.start()
    ht[...] = h[...].T

    def need(n):
        if n > 0:
            dcopy[n - 1].wait()

    tgt = t_ref[...] - lax.axis_index("fsdp") * vloc
    _bwd_chunk(w, h, ht, lse_ref, tgt, dw, dht, (z0, z1), (g0, g1), UN_L, need=need, done=done, scale=1.0 / total)
    for c in recv:
        c.wait()
    dh_ref[...] = dht[...].T + (x[...] + s[...])
    for c in flush:
        c.wait()


def solution(mesh):
    groups = mesh.shape["fsdp"]
    tok_spec = P(("dp", "fsdp"), None)

    def local_head(hidden, targets, weight):
        tok, depth = hidden.shape
        vloc = weight.shape[0]
        total = tok * groups
        half = tok // 2
        vm = pltpu.VMEM
        dma = pltpu.SemaphoreType.DMA
        hbm = pl.BlockSpec(memory_space=pl.ANY)
        loc = pl.BlockSpec(memory_space=pltpu.VMEM)
        np_f = len(_pieces(vloc // SUB, vloc % SUB, UN_O))
        nl = len(_done_pieces(vloc, UN_L))
        sds = jax.ShapeDtypeStruct
        work = [vm((SUB, tok), f32), vm((SUB, tok), f32), vm((SUB, tok), bf16), vm((SUB, tok), bf16)]
        nd = len(_done_pieces(vloc, UN_B))
        dwp, w, h0, x, s, lse, loss = pl.pallas_call(
            lambda *refs: _exchange_kernel(total, *refs),
            in_specs=[hbm, hbm, hbm],
            out_specs=[hbm, loc, loc, hbm, hbm, loc, loc],
            out_shape=[
                sds((vloc, depth), f32), vm((vloc, depth), bf16), vm((tok, depth), bf16),
                sds((tok, depth), f32), sds((tok, depth), f32), vm((1, tok), f32), sds((1, 128), f32),
            ],
            scratch_shapes=[
                vm((vloc, depth), f32), vm((groups - 1, tok, depth), bf16), vm((depth, tok), bf16), vm((groups - 1, depth, tok), bf16),
                vm((depth, tok), f32), vm((3, tok, depth), f32), vm((2, half, depth), f32),
                vm((8, 1, half), jnp.int32), vm((32, 1, half), f32), vm((4, 1, 128), f32), vm((4, 1, tok), f32),
            ] + work + [vm((8, tok), f32)] * 6 + [
                dma((np_f,)), dma((2,)), dma((5,)), dma((5,)), dma, dma, dma, dma((4,)), dma((5,)), dma((5,)), dma, dma, dma((nd,)),
            ],
            compiler_params=pltpu.CompilerParams(vmem_limit_bytes=VMEM_X, collective_id=0, has_side_effects=True),
            name="ce_exchange",
        )(hidden, targets.reshape(2, 1, half), weight)
        keep = lambda a: pltpu.with_memory_space_constraint(a, pltpu.VMEM)
        grad_w, dh = pl.pallas_call(
            lambda *refs: _own_kernel(total, *refs),
            in_specs=[hbm, loc, loc, hbm, hbm, loc, loc],
            out_specs=[hbm, loc],
            out_shape=[sds((vloc, depth), f32), sds((tok, depth), f32)],
            scratch_shapes=[vm((vloc, depth), f32), vm((tok, depth), f32), vm((tok, depth), f32), vm((depth, tok), bf16), vm((depth, tok), f32)]
            + work + [dma((nl,)), dma((nl,)), dma((2,))],
            compiler_params=pltpu.CompilerParams(vmem_limit_bytes=VMEM_L),
            name="ce_own",
        )(dwp, *[keep(a) for a in (w, h0)], x, s, targets[None, :], keep(lse))
        return loss[0, :1], dh, grad_w

    return jax.shard_map(local_head, mesh=mesh, in_specs=(tok_spec, P(("dp", "fsdp")), P("fsdp", None)), out_specs=(P("dp"), tok_spec, tok_spec), check_vma=False)
```

```python
import jax
import jax.numpy as jnp
from jax import lax
from jax.experimental import pallas as pl
from jax.experimental.pallas import tpu as pltpu
from jax.sharding import PartitionSpec as P

SUB = 256
UN_O = 4
UN_F = 14
UN_B = 14
UN_L = 4
VMEM_X = 56_500_000
VMEM_L = 56_500_000
f32 = jnp.float32
bf16 = jnp.bfloat16
MESH = pl.DeviceIdType.MESH


def _nn(a, b):
    return lax.dot_general(a, b, (((1,), (0,)), ((), ())), preferred_element_type=f32)


def _tn(a, b):
    return lax.dot_general(a, b, (((0,), (0,)), ((), ())), preferred_element_type=f32)


def _pieces(full, rem, unroll):
    loops = (full - 2) // unroll
    cuts = [0, 2 * SUB] + [(2 + (i + 1) * unroll) * SUB for i in range(loops)] + [full * SUB + rem]
    return [(a, b - a) for a, b in zip(cuts[:-1], cuts[1:])]


def _fwd_chunk(w, h, ht, zb, mb, s8, un, tgt=None, zt8=None, mid=None, need=None, clear=None):
    vloc = w.shape[0]
    tok = h.shape[0]
    full, rem = vloc // SUB, vloc % SUB
    loops = (full - 2) // un
    ht[...] = h[...].T
    mb[1][...] = jnp.full(mb[1].shape, -jnp.inf, f32)
    s8[...] = jnp.zeros(s8.shape, f32)

    def zdot(k, slot, rows=SUB):
        z = _nn(w[pl.ds(k * SUB, rows), :], ht[...])
        zb[slot][pl.ds(0, rows), :] = z
        mb[slot][...] = jnp.maximum(mb[1 - slot][...], jnp.max(z.reshape(rows // 8, 8, tok), axis=0))

    def epi(k, slot, rows=SUB):
        z = zb[slot][pl.ds(0, rows), :].reshape(rows // 8, 8, tok)
        new = mb[slot][...]
        s8[...] = s8[...] * jnp.exp(mb[2][...] - new) + jnp.sum(jnp.exp(z - new[None]), axis=0)
        mb[2][...] = new
        if clear is not None:
            clear[pl.ds(k * SUB, rows), :] = jnp.zeros((rows, clear.shape[1]), f32)
        if tgt is not None:
            t = tgt - k * SUB
            lane = lax.broadcasted_iota(jnp.int32, (8, tok), 0)
            acc = zt8[...]
            for r in range(rows // 8):
                acc = jnp.where(lane + r * 8 == t, z[r], acc)
            zt8[...] = acc

    def step(k, par, zrows=SUB, erows=SUB):
        if zrows:
            zdot(k + 1, 1 - par, zrows)
        if erows:
            epi(k, par, erows)

    mb[2][...] = mb[1][...]
    if need is not None:
        need(0)
    zdot(0, 0)
    step(0, 0)

    @pl.loop(0, loops)
    def _(i):
        if need is not None:
            for n in range(loops):
                pl.when(i == n)(lambda n=n: need(1 + n))
        for u in range(un):
            step(1 + i * un + u, (1 + u) % 2)
        if mid is not None:
            pl.when(i == 0)(mid)

    if need is not None:
        need(1 + loops)
    for k in range(1 + loops * un, full - 1):
        step(k, k % 2)
    step(full - 1, (full - 1) % 2, zrows=rem)
    step(full, full % 2, zrows=0, erows=rem)
    m8 = mb[2][...]
    top = jnp.max(m8, axis=0, keepdims=True)
    return top + jnp.log(jnp.sum(s8[...] * jnp.exp(m8 - top), axis=0, keepdims=True))


def _bwd_chunk(w, h, ht, lse, tgt, dw, dht, zb, gb, un, zt8=None, mid=None, late=None, need=None, done=None, scale=1.0):
    vloc = w.shape[0]
    tok = h.shape[0]
    full, rem = vloc // SUB, vloc % SUB
    loops = (full - 2) // un

    def zdot(k, slot, rows=SUB):
        zb[slot][pl.ds(0, rows), :] = _nn(w[pl.ds(k * SUB, rows), :], ht[...])

    def epi(k, slot, rows=SUB):
        z = zb[slot][pl.ds(0, rows), :]
        hit = lax.broadcasted_iota(jnp.int32, (rows, tok), 0) == tgt[...] - k * SUB
        p = jnp.exp(z - lse[...])
        if zt8 is not None:
            zt8[...] += jnp.sum(jnp.where(hit, z, 0.0).reshape(rows // 8, 8, tok), axis=0)
        gb[slot][pl.ds(0, rows), :] = ((p - jnp.where(hit, 1.0, 0.0)) * scale).astype(bf16)

    def ddot(k, slot, rows=SUB):
        g = gb[slot][pl.ds(0, rows), :]
        rng = pl.ds(k * SUB, rows)
        dw[rng, :] = dw[rng, :] + _nn(g, h[...])
        dht[...] += _tn(w[rng, :], g)

    def step(k, par, zrows=SUB, erows=SUB, drows=SUB):
        if erows:
            epi(k, par, erows)
        if drows:
            ddot(k - 1, 1 - par, drows)
        if zrows:
            zdot(k + 1, 1 - par, zrows)

    dht[...] = jnp.zeros(dht.shape, f32)
    if need is not None:
        need(0)
    zdot(0, 0)
    step(0, 0, drows=0)
    if mid is not None:
        mid()

    @pl.loop(0, loops)
    def _(i):
        if need is not None:
            for n in range(loops):
                pl.when(i == n)(lambda n=n: need(1 + n))
        for u in range(un):
            step(1 + i * un + u, (1 + u) % 2)
        if late is not None:
            pl.when(i == 0)(late)
        if done is not None:
            for n in range(loops):
                done(n, i == n)

    if need is not None:
        need(1 + loops)
    for k in range(1 + loops * un, full - 1):
        step(k, k % 2)
    step(full - 1, (full - 1) % 2, zrows=rem)
    step(full, full % 2, zrows=0, erows=rem)
    step(full + 1, (full + 1) % 2, zrows=0, erows=0, drows=rem)
    if done is not None:
        done(loops, None)


def _done_pieces(vloc, un):
    full = vloc // SUB
    loops = (full - 2) // un
    cuts = [0] + [(i + 1) * un * SUB for i in range(loops)] + [vloc]
    return [(a, b - a) for a, b in zip(cuts[:-1], cuts[1:])]


def _exchange_kernel(total, h_in, t_in, w_in, dwp, w, h0, x_out, s_out, lse_out, loss_out,
                     dw, hc, ht0, ht, dht, part, ring, tg, lst, zs, lsec, z0, z1, g0, g1, ma, mb_, mc, s8, zt8, ztf,
                     wsem, lsem, hsend, hrecv, tsend, trecv, stsend, strecv, psend, precv, zsend, zrecv, osem):
    vloc, depth = w_in.shape
    tok = h_in.shape[0]
    half = tok // 2
    me = lax.axis_index("fsdp")
    chip, core = me // 2, me % 2
    sib = 2 * chip + (1 - core)
    far = 2 * (1 - chip) + core
    fars = [2 * (1 - chip), 2 * (1 - chip) + 1]
    base = me * vloc
    dev = lambda d: {"fsdp": d}
    zb, gb, mb = (z0, z1), (g0, g1), (ma, mb_, mc)
    scale = 1.0 / total

    def rcopy(src, dst, ssem, rsem, d):
        return pltpu.make_async_remote_copy(src_ref=src, dst_ref=dst, send_sem=ssem, recv_sem=rsem, device_id=dev(d), device_id_type=MESH)

    def wait_bytes(ref, sem):
        pltpu.make_async_copy(ref, ref, sem).wait()

    pieces = _pieces(vloc // SUB, vloc % SUB, UN_O)
    wcopy = [pltpu.make_async_copy(w_in.at[pl.ds(a, n), :], w.at[pl.ds(a, n), :], wsem.at[i]) for i, (a, n) in enumerate(pieces)]
    own_h = pltpu.make_async_copy(h_in, h0, lsem.at[0])
    own_t = pltpu.make_async_copy(t_in, tg.at[pl.ds(0, 2)], lsem.at[1])
    own_h.start()
    own_t.start()
    for c in wcopy:
        c.start()

    barrier = pltpu.get_barrier_semaphore()
    for d in [sib] + fars:
        pl.semaphore_signal(barrier, inc=1, device_id=dev(d), device_id_type=MESH)
    pl.semaphore_wait(barrier, 3)

    mine = pl.ds(core * half, half)
    send_sib = rcopy(h_in, hc.at[0], hsend.at[0], hrecv.at[0], sib)
    send_far = [rcopy(h_in.at[pl.ds(i * half, half), :], hc.at[1 + i, mine, :], hsend.at[1 + i], hrecv.at[1 + i], far) for i in range(2)]
    relay = [rcopy(hc.at[1 + i, mine, :], hc.at[1 + i, mine, :], hsend.at[3 + i], hrecv.at[3 + i], sib) for i in range(2)]
    send_sib.start()
    for c in send_far:
        c.start()
    rcopy(t_in, tg.at[pl.ds(2, 2)], tsend, trecv, sib).start()
    for d in fars:
        for i in range(2):
            rcopy(t_in.at[pl.ds(i, 1)], tg.at[pl.ds(4 + 2 * i + core, 1)], tsend, trecv, d).start()

    zt8[...] = jnp.zeros(zt8.shape, f32)
    ztf[...] = jnp.zeros(ztf.shape, f32)

    def put_stat(pos, v):
        for i in range(2):
            lst[me * 8 + pos * 2 + i] = v[:, i * half:(i + 1) * half]

    def send_stat(pos):
        def go(row, dst_pos, dst_half, d):
            rcopy(lst.at[pl.ds(me * 8 + row, 1)], lst.at[pl.ds(me * 8 + dst_pos * 2 + dst_half, 1)], stsend, strecv.at[dst_pos], d).start()

        near = pos < 2
        for i in range(2):
            go(pos * 2 + i, jnp.where(near, 1 - pos, pos), i, sib)
            for k in range(2):
                go(
                    pos * 2 + i,
                    jnp.where(near, 2 + i, jnp.where(k == i, 0, 1)),
                    jnp.where(near, jnp.where(pos == 0, core, 1 - core), pos - 2),
                    fars[k],
                )

    own_h.wait()
    own_t.wait()
    tg0 = jnp.concatenate([tg[0], tg[1]], axis=1) - base
    put_stat(0, _fwd_chunk(w, h0, ht0, zb, mb, s8, UN_O, tgt=tg0, zt8=ztf, need=lambda n: wcopy[n].wait(), clear=dw))
    send_stat(0)

    @pl.loop(1, 4)
    def _(pos):
        @pl.when(pos == 1)
        def _():
            send_sib.wait_recv()

        for i in range(2):
            @pl.when(pos == 2 + i)
            def _():
                relay[i].wait_recv()

        def forward():
            for i in range(2):
                @pl.when(pos == 1 + i)
                def _():
                    send_far[i].wait_recv()
                    relay[i].start()

        put_stat(pos, _fwd_chunk(w, hc.at[pos - 1], ht.at[pos - 1], zb, mb, s8, UN_F, mid=forward))
        send_stat(pos)

    wait_bytes(tg.at[pl.ds(2, 6)], trecv)

    def join_stat(pos):
        rows = [[lst[s * 8 + pos * 2 + i] for s in range(4)] for i in range(2)]
        out = []
        for r in rows:
            top = jnp.maximum(jnp.maximum(r[0], r[1]), jnp.maximum(r[2], r[3]))
            out.append(top + jnp.log(sum(jnp.exp(x - top) for x in r)))
        return jnp.concatenate(out, axis=1)

    dpieces = _done_pieces(vloc, UN_B)
    flush = [pltpu.make_async_copy(dw.at[pl.ds(a, n), :], dwp.at[pl.ds(a, n), :], osem.at[i]) for i, (a, n) in enumerate(dpieces)]
    theirs = pl.ds((1 - core) * half, half)
    swap = [rcopy(part.at[i, theirs, :], ring.at[i], psend.at[i], precv.at[i], sib) for i in range(2)]
    cross = [rcopy(part.at[i, mine, :], x_out.at[pl.ds(i * half, half), :], psend.at[2 + i], precv.at[2 + i], far) for i in range(2)]
    last = rcopy(dht, s_out, psend.at[4], precv.at[4], sib)

    lsum = jnp.zeros((1, tok), f32)

    @pl.loop(0, 3)
    def _(i):
        pos = lax.rem(i + 1, 3) + 1
        for q in range(3):
            @pl.when(i == q)
            def _():
                wait_bytes(lst.at[pl.ds(0, 6)], strecv.at[(2, 3, 1)[q]])

        lse = join_stat(pos)
        lsec[pl.ds(pos, 1)] = lse[None]
        tpos = jnp.concatenate([tg[pos * 2], tg[pos * 2 + 1]], axis=1) - base

        def combine(q):
            @pl.when(i == q + 1)
            def _():
                swap[q].wait_recv()
                for j in range(4):
                    rows = pl.ds(core * half + j * (half // 4), half // 4)
                    part[q, rows, :] += ring[q, pl.ds(j * (half // 4), half // 4), :]
                cross[q].start()

        def done(n, cond):
            pl.when(i == 2 if cond is None else jnp.logical_and(cond, i == 2))(lambda: flush[n].start())

        _bwd_chunk(w, hc.at[pos - 1], ht.at[pos - 1], lse, tpos, dw, dht, zb, gb, UN_B, zt8=zt8, mid=lambda: combine(1), late=lambda: combine(0), done=done, scale=scale)
        for q in range(2):
            @pl.when(i == q)
            def _():
                part[q] = dht[...].T
                swap[q].start()

    last.start()
    wait_bytes(lst.at[pl.ds(0, 6)], strecv.at[0])
    lsec[0] = join_stat(0)
    lse_out[...] = lsec[0]
    zsum = jnp.sum(zt8[...] + ztf[...], keepdims=True)
    zs[me] = jnp.broadcast_to(zsum, (1, 128))
    for d in [sib] + fars:
        rcopy(zs.at[pl.ds(me, 1)], zs.at[pl.ds(me, 1)], zsend, zrecv, d).start()
    lsum = jnp.sum(lsec[0] + lsec[1] + lsec[2] + lsec[3], keepdims=True)
    wait_bytes(zs.at[pl.ds(0, 3)], zrecv)
    loss_out[...] = (lsum - (zs[0] + zs[1] + zs[2] + zs[3])) * scale
    wait_bytes(zs.at[pl.ds(0, 3)], zsend)
    wait_bytes(lst.at[pl.ds(0, 24)], stsend)
    wait_bytes(tg.at[pl.ds(0, 6)], tsend)
    for c in [send_sib] + send_far + relay + swap:
        c.wait_send()
    for c in flush:
        c.wait()
    for c in cross + [last]:
        c.wait()


def _own_kernel(total, dwp, w, h, x_in, s_in, t_ref, lse_ref, dwo, dh_ref, dw, x, s, ht, dht, z0, z1, g0, g1, dsem, osem, lsem):
    vloc = w.shape[0]
    dpieces = _done_pieces(vloc, UN_L)
    dcopy = [pltpu.make_async_copy(dwp.at[pl.ds(a, n), :], dw.at[pl.ds(a, n), :], dsem.at[i]) for i, (a, n) in enumerate(dpieces)]
    flush = [pltpu.make_async_copy(dw.at[pl.ds(a, n), :], dwo.at[pl.ds(a, n), :], osem.at[i]) for i, (a, n) in enumerate(dpieces)]

    def done(n, cond):
        if cond is None:
            flush[n].start()
        else:
            pl.when(cond)(lambda: flush[n].start())

    recv = [pltpu.make_async_copy(x_in, x, lsem.at[0]), pltpu.make_async_copy(s_in, s, lsem.at[1])]
    for c in dcopy + recv:
        c.start()
    ht[...] = h[...].T

    def need(n):
        if n > 0:
            dcopy[n - 1].wait()

    tgt = t_ref[...] - lax.axis_index("fsdp") * vloc
    _bwd_chunk(w, h, ht, lse_ref, tgt, dw, dht, (z0, z1), (g0, g1), UN_L, need=need, done=done, scale=1.0 / total)
    for c in recv:
        c.wait()
    dh_ref[...] = (dht[...] + s[...]).T + x[...]
    for c in flush:
        c.wait()


def solution(mesh):
    groups = mesh.shape["fsdp"]
    tok_spec = P(("dp", "fsdp"), None)

    def local_head(hidden, targets, weight):
        tok, depth = hidden.shape
        vloc = weight.shape[0]
        total = tok * groups
        half = tok // 2
        vm = pltpu.VMEM
        dma = pltpu.SemaphoreType.DMA
        hbm = pl.BlockSpec(memory_space=pl.ANY)
        loc = pl.BlockSpec(memory_space=pltpu.VMEM)
        np_f = len(_pieces(vloc // SUB, vloc % SUB, UN_O))
        nl = len(_done_pieces(vloc, UN_L))
        sds = jax.ShapeDtypeStruct
        work = [vm((SUB, tok), f32), vm((SUB, tok), f32), vm((SUB, tok), bf16), vm((SUB, tok), bf16)]
        nd = len(_done_pieces(vloc, UN_B))
        dwp, w, h0, x, s, lse, loss = pl.pallas_call(
            lambda *refs: _exchange_kernel(total, *refs),
            in_specs=[hbm, hbm, hbm],
            out_specs=[hbm, loc, loc, hbm, hbm, loc, loc],
            out_shape=[
                sds((vloc, depth), f32), vm((vloc, depth), bf16), vm((tok, depth), bf16),
                sds((tok, depth), f32), sds((depth, tok), f32), vm((1, tok), f32), sds((1, 128), f32),
            ],
            scratch_shapes=[
                vm((vloc, depth), f32), vm((groups - 1, tok, depth), bf16), vm((depth, tok), bf16), vm((groups - 1, depth, tok), bf16),
                vm((depth, tok), f32), vm((2, tok, depth), f32), vm((2, half, depth), f32),
                vm((8, 1, half), jnp.int32), vm((32, 1, half), f32), vm((4, 1, 128), f32), vm((4, 1, tok), f32),
            ] + work + [vm((8, tok), f32)] * 6 + [
                dma((np_f,)), dma((2,)), dma((5,)), dma((5,)), dma, dma, dma, dma((4,)), dma((5,)), dma((5,)), dma, dma, dma((nd,)),
            ],
            compiler_params=pltpu.CompilerParams(vmem_limit_bytes=VMEM_X, collective_id=0, has_side_effects=True),
            name="ce_exchange",
        )(hidden, targets.reshape(2, 1, half), weight)
        keep = lambda a: pltpu.with_memory_space_constraint(a, pltpu.VMEM)
        grad_w, dh = pl.pallas_call(
            lambda *refs: _own_kernel(total, *refs),
            in_specs=[hbm, loc, loc, hbm, hbm, loc, loc],
            out_specs=[hbm, loc],
            out_shape=[sds((vloc, depth), f32), sds((tok, depth), f32)],
            scratch_shapes=[vm((vloc, depth), f32), vm((tok, depth), f32), vm((depth, tok), f32), vm((depth, tok), bf16), vm((depth, tok), f32)]
            + work + [dma((nl,)), dma((nl,)), dma((2,))],
            compiler_params=pltpu.CompilerParams(vmem_limit_bytes=VMEM_L),
            name="ce_own",
        )(dwp, *[keep(a) for a in (w, h0)], x, s, targets[None, :], keep(lse))
        return loss[0, :1], dh, grad_w

    return jax.shard_map(local_head, mesh=mesh, in_specs=(tok_spec, P(("dp", "fsdp")), P("fsdp", None)), out_specs=(P("dp"), tok_spec, tok_spec), check_vma=False)
```
